32 devices in a mesh: dom: 8 (over z, x), feat: 4 (over y, core).
Axes of the slice: x: 2, y: 2, z: 4, core: 2. Of those that a mesh axis runs over, the one named last changes fastest.
Arguments:
- feats: bfloat16 [256, 4096], P('feat', 'dom'), may hold values from -6 to 6
- self_weight: bfloat16 [256, 256], P(None, 'feat'), may hold values from -0.375 to 0.375
- bases: bfloat16 [30, 256, 256], P(None, 'feat'), may hold values from -0.375 to 0.375
- coef: float32 [237, 30], replicated, may hold values from -1.2 to 1.2
- src_part: int32 [8192, 1], P('dom'), may hold values from 0 to 7; in each aligned block of 1024 rows (0 to 1023, 1024 to 2047, ...) at most 256 rows name the same one
- src_row: int32 [8192], P('dom'), may hold values from 0 to 511
- edge_dst: int32 [8192], P('dom'), may hold values from 0 to 511
- edge_rel: int32 [8192], P('dom'), may hold values from 0 to 236
- block_owner: int32 [64, 1], P('dom'), may hold values from 0 to 7; in each aligned block of 8 rows (0 to 7, 8 to 15, ...) at most 2 rows name the same one
- block_valid: int32 [8, 8], P('dom'), may hold values from 1 to 128, 896 in all within a row
- cotangent: bfloat16 [256, 4096], P('feat', 'dom'), may hold values from -6 to 6
Outputs:
- output: bfloat16 [256, 4096], P('feat', 'dom')
- grad_feats: bfloat16 [256, 4096], P('feat', 'dom')
- grad_bases: float32 [30, 256, 256], P(None, 'feat')
- grad_self: float32 [256, 256], P(None, 'feat')
- grad_coef: float32 [237, 30], replicated
The draws below stay inside these ranges and needn't reach their ends.
Inputs may be any that keep to these rules, and one draw needn't show every extreme that they name: `src_part`: among the edge rows of one index of dom, no partition is the source partition of more than 256 rows, and some partition of exactly 256. `block_owner`: among the blocks of one index of dom, no partition owns more than 2, a bound that some block reaches. `block_valid`: the valid rows of a block come first; the counts of one index of dom sum to 896.
All inputs are finite; a program needn't handle non-finite values.
Results may differ from the reference program's by a relative error of at most 0.0055.
Values may be sent and summed in bfloat16 or wider, within the bound.
A program may use at most 64 MiB of HBM per device.

```python
import math
import jax
import jax.numpy as jnp
import numpy as np
from jax import lax

D = 256
BASES = 30
RELS = 237
ROWS = 128
ENT_DEV = 512
NB = 8
EDGE_DEV = 1024
ENTITIES = 4096
EDGES = 8192
BLOCKS = 64
SCAP = 256
BCAP = 2
VALID_DEV = 896
N_DOM = 8


def set_ends(result, own_key, smallest, top_value):
    longest = result.shape.index(max(result.shape))
    spots = []
    for shift in (0, 1):
        where = [jax.random.randint(jax.random.fold_in(own_key, axis), (), 0, length) for axis, length in enumerate(result.shape)]
        where[longest] = (where[longest] + shift) % result.shape[longest]
        spots.append(tuple(where))
    return result.at[spots[0]].set(smallest).at[spots[1]].set(top_value)


def shard_levels(own_key, extent, pieces, least, high):
    factor_of = 1.0
    for position, shards_of in pieces:
        steps = jax.random.uniform(jax.random.fold_in(jax.random.fold_in(own_key, 6), position), (shards_of,), jnp.float32, least / len(pieces), high / len(pieces))
        factor_of = factor_of * jnp.repeat(jnp.exp(steps), extent[position] // shards_of).reshape((-1,) + (1,) * (len(extent) - 1 - position))
    return factor_of


def rank_bounds(amount, lean):
    loads = [(1 << 20) // math.isqrt(rank ** lean) + 1 for rank in range(1, amount + 1)]
    scale = 1 + sum(loads) // (1 << 30)
    return np.cumsum(np.array([max(1, weight // scale) for weight in loads]))


def skewed_ids(rng, extent, number_of, skew):
    grid = rank_bounds(number_of, skew)
    lot = jax.random.randint(jax.random.fold_in(rng, 1), extent, 0, int(grid[number_of - 1]))
    grade = jnp.searchsorted(jnp.asarray(grid, jnp.int32), lot, side="right")
    return jax.random.permutation(jax.random.fold_in(rng, 2), number_of)[grade].astype(jnp.int32)


def length_profile(amount, total, most, skew):
    loads = [(1 << 20) // math.isqrt(grade ** skew) + 1 for grade in range(2, amount + 1)]
    rest, given = total - most - (amount - 1), [1] * (amount - 1)
    while rest > 0:
        movable = [i for i in range(amount - 1) if given[i] < most]
        whole, remaining = sum([loads[i] for i in movable]), rest
        for i in movable:
            addition = min(most - given[i], max(1, remaining * loads[i] // whole), rest)
            given[i] = given[i] + addition
            rest = rest - addition
    return np.array([most] + given)


def uneven_parts(own_key, count, total, bound, slope):
    if count == 2:
        one = jax.random.randint(own_key, (), max(1, total - bound), min(bound, total - 1) + 1)
        return jnp.stack([one, total - one])
    sizes = jnp.asarray(length_profile(count, total, bound, slope), jnp.int32)
    couples = (count - 1) // 2
    source_of, sink = sizes[1:1 + 2 * couples:2], sizes[2:2 + 2 * couples:2]
    margin = jnp.minimum(source_of - 1, bound - sink)
    shifted = jax.random.randint(jax.random.fold_in(own_key, 1), (couples,), 0, 1 << 20) % (margin + 1)
    sizes = sizes.at[1:1 + 2 * couples:2].set(source_of - shifted).at[2:2 + 2 * couples:2].set(sink + shifted)
    return sizes[jax.random.permutation(jax.random.fold_in(own_key, 2), count)]


def deal_out(own_key, own, number, rows, number_of, top, limit, slope):
    order = jax.random.permutation(own_key, number_of)
    packed, ordinary = load_shares(number_of, rows * top, limit, slope, True), load_shares(number_of, rows * top, limit, slope, False)
    places = jnp.arange(number_of)

    def named(tallies, rotation):
        used = int((tallies > 0).sum())
        fixed = max(1, used // 4)
        moved = fixed + (places - fixed + rotation * (used - fixed)) % max(1, number_of - fixed)
        return jnp.zeros((number_of,), jnp.int32).at[order[jnp.where(places < fixed, places, moved)]].set(jnp.asarray(tallies, jnp.int32))

    tallies = jnp.where(number % 4 == 0, named(packed, number // 4), named(ordinary, number - number // 4 - 1))
    mixed = jax.random.permutation(jax.random.fold_in(own, 3), number_of)
    giver, receiver = mixed[0:number_of // 2 * 2:2], mixed[1:number_of // 2 * 2:2]
    room = jnp.minimum(tallies[giver] - 1, limit - tallies[receiver]) // 2
    room = jnp.where((giver == order[0]) | (receiver == order[0]) | (tallies[receiver] == 0), 0, jnp.maximum(room, 0))
    moved = jax.random.randint(jax.random.fold_in(own, 4), (number_of // 2,), 0, 1 << 20) % (room + 1)
    tallies = tallies.at[giver].add(-moved).at[receiver].add(moved)
    labels = jnp.searchsorted(jnp.cumsum(tallies), jnp.arange(rows * top), side="right").astype(jnp.int32)
    grid = labels.reshape(top, rows).T
    grid = grid[jax.random.permutation(jax.random.fold_in(own, 1), rows)]
    rotation = jax.random.randint(jax.random.fold_in(own, 2), (rows, 1), 0, top)
    return jnp.take_along_axis(grid, (jnp.arange(top)[None, :] + rotation) % top, axis=1)


def load_shares(count, total, bound, skew, full):
    loads = [(1 << 20) // math.isqrt(standing ** skew) + 1 for standing in range(1, count + 1)]
    largest = bound if full else min(bound, max(-(-total // count), total * loads[0] // sum(loads)))
    least = 1 if total - largest >= count - 1 else 0
    given, rest = [largest] + [least] * (count - 1), total - largest - least * (count - 1)
    while rest > 0:
        free = [i for i in range(1, count) if given[i] < largest] or [i for i in range(1, count) if given[i] < bound]
        mass, remaining = sum([loads[i] for i in free]), rest
        for i in free:
            extra = min(bound - given[i], max(1, remaining * loads[i] // mass), rest)
            given[i] = given[i] + extra
            rest = rest - extra
    return np.array(given)


def normal_values(stream_key, extent, width, bound, pieces=(), held_as=jnp.bfloat16):
    array = jax.random.normal(stream_key, extent, jnp.float32) * width
    if len(pieces) > 0:
        array = shard_levels(stream_key, extent, pieces, -0.22, 0.18) * array
    return jnp.clip(array, min=-bound, max=bound).astype(held_as)


def setup_inputs(seed: int = 0) -> dict:
    key_list = jax.random.split(jax.random.key(seed), 12)
    feats = normal_values(key_list[0], (D, ENTITIES), 1.0, 6.0, ((0, 4), (1, 8)))
    self_weight = normal_values(key_list[1], (D, D), D ** -0.5, 0.375, ((1, 4),))
    bases = normal_values(key_list[2], (BASES, D, D), D ** -0.5, 0.375, ((1, 4),))
    coef = normal_values(key_list[3], (RELS, BASES), 0.2, 1.2, (), jnp.float32)
    src_part_keys = jax.random.split(jax.random.fold_in(key_list[4], 1), EDGES // EDGE_DEV)
    src_part_turns = jax.random.permutation(jax.random.fold_in(key_list[4], 3), EDGES // EDGE_DEV)
    src_part = jax.vmap(lambda own, number: deal_out(jax.random.fold_in(key_list[4], 2), own, number, EDGE_DEV, N_DOM, 1, SCAP, 2))(src_part_keys, src_part_turns).reshape((EDGES, 1))
    src_row = set_ends(jax.random.randint(key_list[5], (EDGES,), 0, ENT_DEV), jax.random.fold_in(key_list[5], 1), 0, ENT_DEV - 1).astype(jnp.int32)
    edge_dst = set_ends(jax.random.randint(key_list[6], (EDGES,), 0, ENT_DEV), jax.random.fold_in(key_list[6], 1), 0, ENT_DEV - 1).astype(jnp.int32)
    edge_rel = set_ends(skewed_ids(key_list[7], (EDGES,), RELS, 2), jax.random.fold_in(key_list[7], 3), 0, RELS - 1).astype(jnp.int32)
    block_owner_keys = jax.random.split(jax.random.fold_in(key_list[8], 1), BLOCKS // NB)
    block_owner_turns = jax.random.permutation(jax.random.fold_in(key_list[8], 3), BLOCKS // NB)
    block_owner = jax.vmap(lambda own, number: deal_out(jax.random.fold_in(key_list[8], 2), own, number, NB, N_DOM, 1, BCAP, 2))(block_owner_keys, block_owner_turns).reshape((BLOCKS, 1))
    block_valid = jax.vmap(lambda own: uneven_parts(own, NB, VALID_DEV, ROWS, 2))(jax.random.split(key_list[9], N_DOM)).reshape((N_DOM, NB)).astype(jnp.int32)
    cotangent = normal_values(key_list[10], (D, ENTITIES), 1.0, 6.0, ((0, 4), (1, 8)))
    return dict(feats=feats, self_weight=self_weight, bases=bases, coef=coef, src_part=src_part, src_row=src_row, edge_dst=edge_dst, edge_rel=edge_rel, block_owner=block_owner, block_valid=block_valid, cotangent=cotangent)


def float_dot(left, right):
    return jnp.dot(left.astype(jnp.float32), right.astype(jnp.float32), precision=lax.Precision.HIGHEST)


def reference(feats, self_weight, bases, coef, src_part, src_row, edge_dst, edge_rel, block_owner, block_valid, cotangent):
    entity_total = ENT_DEV * N_DOM
    edge_total = EDGE_DEV * N_DOM
    source_ids = (src_part[:, 0] * ENT_DEV + src_row).astype(jnp.int32)
    owners = jnp.repeat(block_owner[:, 0], ROWS)
    live_rows = (jnp.arange(ROWS, dtype=jnp.int32)[None, :] < block_valid.reshape(-1)[:, None]).reshape(-1)
    target_ids = (owners * ENT_DEV + edge_dst).astype(jnp.int32)
    live_float = live_rows.astype(jnp.float32)
    degree = jnp.zeros((entity_total,), jnp.float32).at[target_ids].add(live_float)
    inverse_degree = 1.0 / jnp.maximum(degree, 1.0)
    edge_coef = coef[edge_rel]
    bases_flat = jnp.transpose(bases, (2, 0, 1)).reshape(D, BASES * D).astype(jnp.float32)
    grouped = (source_ids.reshape(N_DOM, EDGE_DEV), target_ids.reshape(N_DOM, EDGE_DEV),
               edge_coef.reshape(N_DOM, EDGE_DEV, BASES), live_float.reshape(N_DOM, EDGE_DEV),
               edge_rel.reshape(N_DOM, EDGE_DEV))

    def basis_products(src_ids):
        source_feats = feats[:, src_ids].astype(jnp.float32)
        products = jnp.dot(source_feats.T, bases_flat, precision=lax.Precision.HIGHEST)
        return source_feats, products.reshape(-1, BASES, D)

    def forward_group(aggregate, group):
        src_ids, dst_ids, weights, live, rels = group
        source_feats, products = basis_products(src_ids)
        message = jnp.einsum("eb,ebo->eo", weights, products, precision=lax.Precision.HIGHEST)
        message = (message * live[:, None]).astype(jnp.bfloat16)
        return aggregate.at[dst_ids].add(message.astype(jnp.float32)), jnp.zeros((), jnp.float32)

    aggregate, ignored = lax.scan(forward_group, jnp.zeros((entity_total, D), jnp.float32), grouped)
    preact = float_dot(feats.T, self_weight) + inverse_degree[:, None] * aggregate
    output = jax.nn.silu(preact).astype(jnp.bfloat16)
    sigmoid_pre = jax.nn.sigmoid(preact)
    grad_pre = (cotangent.T.astype(jnp.float32) * sigmoid_pre * (1.0 + preact * (1.0 - sigmoid_pre))).astype(jnp.bfloat16)

    def backward_group(totals_now, group):
        grad_bases, grad_coef, edge_grads = totals_now
        src_ids, dst_ids, weights, live, rels = group
        source_feats, products = basis_products(src_ids)
        grad_message = inverse_degree[dst_ids][:, None] * grad_pre[dst_ids].astype(jnp.float32) * live[:, None]
        grad_message = grad_message.astype(jnp.bfloat16).astype(jnp.float32)
        scaled = jnp.einsum("ebo,eo->eb", products, grad_message, precision=lax.Precision.HIGHEST)
        grad_coef = grad_coef + jax.ops.segment_sum(scaled, rels, num_segments=RELS)
        combined = (weights[:, :, None] * grad_message[:, None, :]).astype(jnp.bfloat16).reshape(-1, BASES * D)
        grad_bases = grad_bases + float_dot(source_feats, combined)
        edge_part = float_dot(combined, bases_flat.T)
        edge_grads = edge_grads.at[src_ids].add(edge_part)
        return (grad_bases, grad_coef, edge_grads), jnp.zeros((), jnp.float32)

    start_state = (jnp.zeros((D, BASES * D), jnp.float32), jnp.zeros((RELS, BASES), jnp.float32),
                   jnp.zeros((entity_total, D), jnp.float32))
    final_state, ignored = lax.scan(backward_group, start_state, grouped)
    grad_bases, grad_coef, edge_grads = final_state
    self_part = float_dot(grad_pre, self_weight.T)
    grad_feats = (self_part + edge_grads).astype(jnp.bfloat16).T
    grad_self = float_dot(feats, grad_pre)
    scale = float(edge_total) ** -0.5
    grad_bases = jnp.transpose((grad_bases * scale).reshape(D, BASES, D), (1, 2, 0))
    return (output.T, grad_feats, grad_bases, grad_self * scale, grad_coef * scale)
```

```python
from types import SimpleNamespace

import jax
import jax.numpy as jnp
from jax import lax
from jax.experimental import pallas as pl
from jax.experimental.pallas import tpu as pltpu
from jax.sharding import PartitionSpec as P

BF = jnp.bfloat16
F32 = jnp.float32
I32 = jnp.int32
LANES = 128
DOM, FEAT = "dom", "feat"


def dot(left, right, left_axis, right_axis):
    return lax.dot_general(
        left, right, (((left_axis,), (right_axis,)), ((), ())), preferred_element_type=F32
    )


def each(start, stop, step):
    if stop - start <= 8:
        for index in range(start, stop):
            step(index)
    else:
        lax.fori_loop(start, stop, lambda index, carry: (step(index), carry)[1], 0)


def peers(axis, count):
    me = lax.axis_index(axis)
    return me, me // 2, me % 2, count // 2


def greet(groups):
    barrier = pltpu.get_barrier_semaphore()
    for axis, count in groups:
        me = lax.axis_index(axis)

        def hello(hop):
            pl.semaphore_signal(
                barrier,
                inc=1,
                device_id={axis: (me + hop) % count},
                device_id_type=pl.DeviceIdType.MESH,
            )

        each(1, count, hello)
    return lambda: pl.semaphore_wait(barrier, sum(count - 1 for axis, count in groups))


def remote(source, target_ref, send_sem, recv_sem, axis, target):
    return pltpu.make_async_remote_copy(
        src_ref=source,
        dst_ref=target_ref,
        send_sem=send_sem,
        recv_sem=recv_sem,
        device_id={axis: target},
        device_id_type=pl.DeviceIdType.MESH,
    )


class Gather:
    def __init__(self, axis, count, source, table, sems):
        self.me, self.spot, self.side, self.columns = peers(axis, count)
        self.axis, self.source, self.table = axis, source, table
        self.sends, self.recvs, self.pair_sends, self.pair_recvs = sems

    def direct(self, hop):
        target = (self.spot + hop) % self.columns * 2 + self.side
        return remote(
            self.source,
            self.table(self.me),
            self.sends.at[hop - 1],
            self.recvs.at[hop - 1],
            self.axis,
            target,
        )

    def place(self, hop, side):
        return (self.spot - hop + self.columns) % self.columns * 2 + side

    def relay(self, hop, own=False):
        spot = self.table(self.place(hop, self.side))
        return remote(
            self.source if own else spot,
            spot,
            self.pair_sends.at[hop],
            self.pair_recvs.at[hop],
            self.axis,
            self.spot * 2 + 1 - self.side,
        )

    def start(self):
        each(1, self.columns, lambda hop: self.direct(hop).start())
        self.relay(0, True).start()

    def forward(self, hop):
        self.direct(hop).wait_recv()
        self.relay(hop).start()
        return self.place(hop, self.side)

    def from_mate(self, hop):
        self.relay(hop).wait_recv()
        return self.place(hop, 1 - self.side)

    def finish(self):
        each(1, self.columns, lambda hop: self.direct(hop).wait_send())
        each(0, self.columns, lambda hop: self.relay(hop).wait_send())


def gather_sems(count):
    columns = count // 2
    return [columns - 1, columns - 1, columns, columns]


class Swap:
    def __init__(self, axis, count, source, table, sems):
        self.me = lax.axis_index(axis)
        self.axis, self.count, self.source, self.table = axis, count, source, table
        self.sends, self.recvs = sems

    def copy(self, hop):
        target = (self.me + hop) % self.count
        return remote(
            self.source(target),
            self.table(self.me),
            self.sends.at[hop - 1],
            self.recvs.at[hop - 1],
            self.axis,
            target,
        )

    def start(self):
        each(1, self.count, lambda hop: self.copy(hop).start())

    def wait(self, hop):
        self.copy(hop).wait_recv()
        return (self.me - hop + self.count) % self.count

    def finish(self):
        each(1, self.count, lambda hop: self.copy(hop).wait_send())


def swap_sems(count):
    return [count - 1, count - 1]


class Reduce:
    def __init__(self, axis, count, block, landed, summed, arrived, sems):
        self.me, self.spot, self.side, self.columns = peers(axis, count)
        self.axis, self.block = axis, block
        self.landed, self.summed, self.arrived = landed, summed, arrived
        self.sends, self.recvs, self.pair_sends, self.pair_recvs = sems

    def place(self, step):
        return (self.spot + 1 + step) % self.columns

    def passing(self, step):
        return remote(
            self.block(self.place(step) * 2 + 1 - self.side),
            self.landed.at[step],
            self.pair_sends.at[step],
            self.pair_recvs.at[step],
            self.axis,
            self.spot * 2 + 1 - self.side,
        )

    def onward(self, step):
        return remote(
            self.summed.at[step],
            self.arrived.at[step],
            self.sends.at[step],
            self.recvs.at[step],
            self.axis,
            self.place(step) * 2 + self.side,
        )

    def pair(self, step):
        self.passing(step).wait_recv()
        own = self.block(self.place(step) * 2 + self.side)
        return own[...].astype(F32) + self.landed[step].astype(F32)

    def middle(self, step):
        self.summed[step] = self.pair(step).astype(BF)
        self.onward(step).start()

    def finish(self, total):
        total[...] = self.pair(self.columns - 1)

        def add(step):
            self.onward(step).wait_recv()
            total[...] += self.arrived[step].astype(F32)

        each(0, self.columns - 1, add)

    def drain(self):
        each(0, self.columns, lambda step: self.passing(step).wait_send())
        each(0, self.columns - 1, lambda step: self.onward(step).wait_send())


def sem_list(counts):
    return [pltpu.SemaphoreType.DMA((count,)) for count in counts]


def reduce_room(count, shape):
    columns = count // 2
    sizes = (columns, columns - 1, columns - 1)
    return [pltpu.VMEM((size,) + shape, BF) for size in sizes], sem_list(gather_sems(count))


def group_of(count):
    return max(size for size in range(1, 6) if count % size == 0)


def layer(
    feats, weight_t, bases, coef_t, part, row, dst, rel, cotangent, owner, valid, dom, feat
):
    quarter, entities = feats.shape
    width = weight_t.shape[1]
    edges = row.shape[1]
    blocks = valid.shape[1]
    rows = edges // blocks
    basis_count = bases.shape[0]
    relations = coef_t.shape[1]
    cap = max(1, 2 * blocks // dom)
    slots = cap * rows
    rel_pad = -(-relations // 256) * 256
    cut = basis_count * quarter
    total_rows = -(-(cut + quarter) // (16 * dom)) * 16 * dom
    while total_rows % quarter:
        total_rows += 16 * dom
    height = total_rows // dom
    basis_pad = total_rows // quarter
    rotated = height % quarter == 0
    group = height // quarter if rotated else group_of(basis_pad)
    basis_rows = -(-basis_count // 8) * 8
    while basis_rows * rel_pad // LANES % dom:
        basis_rows += 8
    coef_rows = basis_rows * rel_pad // LANES // dom
    chunks = 2
    span = edges // chunks
    scale = float(edges * dom) ** (-0.5)

    room = SimpleNamespace()
    room.bases = pltpu.VMEM((basis_pad, quarter, width), BF)
    room.bases_sems = sem_list([1])
    room.weights = pltpu.VMEM((basis_pad, edges), F32)
    room.rel_hot = pltpu.VMEM((rel_pad, edges), BF)
    room.coef_wide = pltpu.VMEM((basis_rows, rel_pad), F32)
    room.sids = pltpu.VMEM((1, edges), I32)
    room.tids = pltpu.VMEM((blocks, 1, rows), I32)
    room.slot_out = pltpu.VMEM((dom, cap, rows), I32)
    room.slot_in = pltpu.VMEM((dom, cap, rows), I32)
    room.slot_sems = sem_list(swap_sems(dom))
    room.hots = pltpu.VMEM((dom, entities, slots), BF)
    room.degree = pltpu.VMEM((16, entities), F32)
    room.table = pltpu.VMEM((dom, quarter, entities), BF)
    room.table_sems = sem_list(gather_sems(dom))
    room.picked = pltpu.VMEM((quarter, edges), F32)
    room.own = pltpu.VMEM((feat, quarter, entities), BF)
    room.own_sems = sem_list(gather_sems(feat))
    room.sources = pltpu.VMEM((feat, quarter, edges), BF)
    room.source_sems = [sem_list(gather_sems(feat)) for chunk in range(chunks)]
    room.products = pltpu.VMEM((total_rows, edges), BF)
    room.messages = pltpu.VMEM((blocks, quarter, rows), BF)
    room.message_out = pltpu.VMEM((dom, cap, quarter, rows), BF)
    room.message_in = pltpu.VMEM((dom, cap, quarter, rows), BF)
    room.message_sems = sem_list(swap_sems(dom))
    room.preact = pltpu.VMEM((quarter, entities), F32)
    room.aggregate = pltpu.VMEM((quarter, entities), F32)
    room.grad_out = pltpu.VMEM((dom, cap, quarter, rows), BF)
    room.grad_in = pltpu.VMEM((dom * cap, quarter, rows), BF)
    room.grad_sems = sem_list(swap_sems(dom))
    room.grad_message = pltpu.VMEM((quarter, edges), BF)
    room.self_rows = pltpu.VMEM((quarter, width), BF)
    room.self_send = pltpu.VMEM((feat, quarter, entities), BF)
    room.self_reduce = reduce_room(feat, (quarter, entities))
    room.self_sum = pltpu.VMEM((quarter, entities), F32)
    room.stack = pltpu.VMEM((total_rows, width), BF)
    room.stack_reduce = reduce_room(dom, (height, width))
    room.piece = pltpu.VMEM((height, width), F32)
    room.pieces_sems = sem_list(gather_sems(dom))
    room.scaled = pltpu.VMEM((basis_rows, edges), F32)
    room.combined = pltpu.VMEM(((2 if rotated else 1) * group * quarter, edges), BF)
    room.edge_sum = pltpu.VMEM((width, edges), F32)
    room.edge_send = pltpu.VMEM((feat, quarter, edges), BF)
    room.edge_reduce = reduce_room(feat, (quarter, edges))
    room.edge_total = pltpu.VMEM((quarter, edges), F32)
    room.edge_grad = pltpu.VMEM((quarter, edges), BF)
    room.nodes = pltpu.VMEM((dom, quarter, entities), BF)
    room.node_reduce = reduce_room(dom, (quarter, entities))
    room.node_sum = pltpu.VMEM((quarter, entities), F32)
    room.coef_out = pltpu.VMEM((dom, coef_rows, LANES), F32)
    room.coef_in = pltpu.VMEM((dom, coef_rows, LANES), F32)
    room.coef_sems = sem_list(swap_sems(dom))
    room.coef_feat = pltpu.VMEM((feat, coef_rows, LANES), F32)
    room.coef_feat_sems = sem_list(swap_sems(feat))
    room.coef_all_sems = sem_list(swap_sems(dom))

    shapes, tree = jax.tree.flatten(vars(room))

    def kernel(
        feats_ref,
        weight_ref,
        bases_hbm,
        coef_ref,
        part_ref,
        row_ref,
        dst_ref,
        rel_ref,
        cot_ref,
        owner_ref,
        valid_ref,
        output_ref,
        grad_feats_ref,
        pieces_ref,
        coef_all_ref,
        *scratch,
    ):
        at = SimpleNamespace(**jax.tree.unflatten(tree, scratch))

        def reduce_of(space, axis, count, block):
            buffers, sems = space
            return Reduce(axis, count, block, *buffers, sems)

        me = lax.axis_index(DOM)
        fme = lax.axis_index(FEAT)
        met = greet([(DOM, dom), (FEAT, feat)])

        load = pltpu.make_async_copy(
            bases_hbm, at.bases.at[pl.ds(0, basis_count)], at.bases_sems[0].at[0]
        )
        load.start()
        if basis_pad > basis_count:
            extra = basis_pad - basis_count
            at.bases[basis_count:] = jnp.zeros((extra, quarter, width), BF)
        at.sids[...] = part_ref[...] * entities + row_ref[...]
        lane = lax.broadcasted_iota(I32, (1, rows), 1)
        spots = []
        for k in range(blocks):
            ids = dst_ref[:, k * rows:(k + 1) * rows]
            at.tids[k] = jnp.where(lane < valid_ref[0, k], ids, -1)
            rank = 0
            for other in range(k):
                rank = rank + jnp.where(owner_ref[0, other] == owner_ref[0, k], 1, 0)
            spots.append(owner_ref[0, k] * cap + rank)

        def block_at(slot):
            found = -1
            for k in range(blocks):
                found = jnp.where(spots[k] == slot, k, found)
            return found

        def fill(place):
            for j in range(cap):
                found = block_at(place * cap + j)
                used = jnp.where(found >= 0, 1, 0)
                ids = at.tids[jnp.maximum(found, 0)]
                at.slot_out[place, j:j + 1] = ids * used + (used - 1)

        each(0, dom, fill)
        at.slot_in[me] = at.slot_out[me]

        at.coef_wide[...] = jnp.zeros((basis_rows, rel_pad), F32)
        at.coef_wide[:basis_count, :relations] = coef_ref[...]
        wide = at.coef_wide[...]
        first = wide.astype(BF)
        second = (wide - first.astype(F32)).astype(BF)
        third = (wide - first.astype(F32) - second.astype(F32)).astype(BF)
        thirds = jnp.concatenate([first, second, third], axis=0)
        rel_rows = lax.broadcasted_iota(I32, (rel_pad, rows), 0)
        for k in range(blocks):
            lanes = slice(k * rows, (k + 1) * rows)
            at.rel_hot[:, lanes] = jnp.where(rel_rows == rel_ref[:, lanes], 1.0, 0.0).astype(BF)
        three = dot(thirds, at.rel_hot[...], 1, 0)
        weights = three[:basis_rows] + three[basis_rows:2 * basis_rows] + three[2 * basis_rows:]
        if basis_pad <= basis_rows:
            at.weights[...] = weights[:basis_pad]
        else:
            at.weights[:basis_rows] = weights
            at.weights[basis_rows:] = jnp.zeros((basis_pad - basis_rows, edges), F32)
        at.own[fme] = feats_ref[...]

        met()

        table = Gather(
            DOM, dom, feats_ref, lambda place: at.table.at[place], at.table_sems
        )
        slot = Swap(
            DOM,
            dom,
            lambda place: at.slot_out.at[place],
            lambda place: at.slot_in.at[place],
            at.slot_sems,
        )
        slot.start()
        table.start()
        own = Gather(
            FEAT,
            feat,
            at.own.at[fme],
            lambda place: at.own.at[place],
            at.own_sems,
        )
        own.start()

        entity_rows = lax.broadcasted_iota(I32, (entities, edges), 0)

        def hot_of(place):
            hot = entity_rows + place * entities == at.sids[...]
            return jnp.where(hot, 1.0, 0.0).astype(BF)

        def use(place):
            at.picked[...] += dot(at.table[place], hot_of(place), 1, 0)

        at.picked[...] = dot(feats_ref[...], hot_of(me), 1, 0)
        use(table.from_mate(0))
        each(1, own.columns, lambda hop: own.forward(hop))
        each(1, table.columns, lambda hop: use(table.forward(hop)))
        each(1, table.columns, lambda hop: use(table.from_mate(hop)))

        gathers = []
        for chunk in range(chunks):
            lanes = pl.ds(chunk * span, span)
            at.sources[fme, :, lanes] = at.picked[:, lanes].astype(BF)
            gather = Gather(
                FEAT,
                feat,
                at.sources.at[fme, :, lanes],
                lambda place, lanes=lanes: at.sources.at[place, :, lanes],
                at.source_sems[chunk],
            )
            gather.start()
            gathers.append(gather)
        each(0, own.columns, lambda hop: own.from_mate(hop))
        own_full = at.own[...].reshape(width, entities)
        at.preact[...] = dot(weight_ref[...], own_full, 1, 0)
        load.wait()

        def forward(chunk):
            lanes = pl.ds(chunk * span, span)
            sources = at.sources[:, :, lanes].reshape(width, span)
            products = dot(at.bases[...].reshape(total_rows, width), sources, 1, 0)
            at.products[:, lanes] = products.astype(BF)
            total = jnp.zeros((quarter, span), F32)
            for k in range(basis_count):
                total += products[k * quarter:(k + 1) * quarter] * at.weights[k:k + 1, lanes]
            total = total.astype(BF)
            for k in range(span // rows):
                at.messages[chunk * (span // rows) + k] = total[:, k * rows:(k + 1) * rows]

        for gather in gathers:
            each(1, gather.columns, lambda hop: gather.forward(hop))
        for chunk, gather in enumerate(gathers):
            each(0, gather.columns, lambda hop: gather.from_mate(hop))
            forward(chunk)

        message = Swap(
            DOM,
            dom,
            lambda place: at.message_out.at[place],
            lambda place: at.message_in.at[place],
            at.message_sems,
        )

        def load_out(place):
            for j in range(cap):
                found = jnp.maximum(block_at(place * cap + j), 0)
                at.message_out[place, j] = at.messages[found]

        def send_out(hop):
            load_out((me + hop) % dom)
            message.copy(hop).start()

        each(1, dom, send_out)
        load_out(me)
        at.message_in[me] = at.message_out[me]

        slot_rows = lax.broadcasted_iota(I32, (entities, rows), 0)
        ones = jnp.ones((16, slots), BF)

        def slot_hot(place):
            parts = [
                jnp.where(slot_rows == at.slot_in[place, j:j + 1], 1.0, 0.0).astype(BF)
                for j in range(cap)
            ]
            hot = jnp.concatenate(parts, axis=1)
            at.hots[place] = hot
            at.degree[...] += dot(ones, hot, 1, 1)

        at.degree[...] = jnp.zeros((16, entities), F32)
        slot_hot(me)
        each(1, dom, lambda hop: slot_hot(slot.wait(hop)))

        def gather_in(place):
            parts = [at.message_in[place, j] for j in range(cap)]
            value = jnp.concatenate(parts, axis=1)
            return dot(value, at.hots[place], 1, 1)

        at.aggregate[...] = gather_in(me)

        def take(hop):
            at.aggregate[...] += gather_in(message.wait(hop))

        each(1, dom, take)

        inverse = 1.0 / jnp.maximum(at.degree[0:1, :], 1.0)
        preact = at.preact[...] + inverse * at.aggregate[...]
        sigmoid = jax.nn.sigmoid(preact)
        output_ref[...] = (preact * sigmoid).astype(BF)
        grad_pre = (cot_ref[...].astype(F32) * sigmoid * (1.0 + preact * (1.0 - sigmoid))).astype(BF)
        grad_node = (grad_pre.astype(F32) * inverse).astype(BF)

        back = Swap(
            DOM,
            dom,
            lambda place: at.grad_out.at[place],
            lambda place: at.grad_in.at[pl.ds(place * cap, cap)],
            at.grad_sems,
        )

        def slot_grads(place, target):
            value = dot(grad_node, at.hots[place], 1, 0).astype(BF)
            for j in range(cap):
                target[j] = value[:, j * rows:(j + 1) * rows]

        def send_back(hop):
            place = (me + hop) % dom
            slot_grads(place, at.grad_out.at[place])
            back.copy(hop).start()

        each(1, dom, send_back)
        slot_grads(me, at.grad_in.at[pl.ds(me * cap, cap)])

        own_full = at.own[...].reshape(width, entities)
        at.self_rows[...] = dot(grad_pre, own_full, 1, 1).astype(BF)
        at.self_send[...] = (
            dot(weight_ref[...], grad_pre, 0, 0).astype(BF).reshape(feat, quarter, entities)
        )
        self_reduce = reduce_of(at.self_reduce, FEAT, feat, lambda place: at.self_send.at[place])
        each(0, self_reduce.columns, lambda step: self_reduce.passing(step).start())
        at.edge_sum[...] = jnp.zeros((width, edges), F32)

        each(1, dom, lambda hop: back.wait(hop))
        for k in range(blocks):
            at.grad_message[:, k * rows:(k + 1) * rows] = at.grad_in[spots[k]]

        def combine(base, half):
            for chunk in range(chunks):
                lanes = pl.ds(chunk * span, span)
                grad = at.grad_message[:, lanes].astype(F32)
                for k in range(group):
                    weight = at.weights[pl.ds(base + k, 1), lanes]
                    top = (half * group + k) * quarter
                    at.combined[top:top + quarter, lanes] = (grad * weight).astype(BF)
            block = at.combined[half * group * quarter:(half + 1) * group * quarter, :]
            piece = dot(block, at.sources[...].reshape(width, edges), 1, 1)
            start = pl.multiple_of(base * quarter, group * quarter)
            at.stack[pl.ds(start, group * quarter), :] = piece.astype(BF)

            @pl.when(base + group == basis_pad)
            def _():
                at.stack[cut:cut + quarter, :] = at.self_rows[...]

        def part_of(base):
            return at.bases[pl.ds(base, group)].reshape(group * quarter, width)

        def edge_add(parts):
            count = len(parts) * group * quarter
            value = jnp.concatenate(parts, axis=0)
            at.edge_sum[...] += dot(value, at.combined[:count, :], 0, 0)

        stack = reduce_of(
            at.stack_reduce,
            DOM,
            dom,
            lambda place: at.stack.at[pl.ds(pl.multiple_of(place * height, height), height)],
        )
        if rotated:

            def work(step):
                place = stack.place(step)
                other = (place * 2 + 1 - stack.side) * group
                mine = (place * 2 + stack.side) * group
                combine(other, 0)
                stack.passing(step).start()
                combine(mine, 1)
                edge_add([part_of(other), part_of(mine)])

            each(0, stack.columns, work)
        else:

            def whole(index, carry):
                combine(index * group, 0)
                edge_add([part_of(index * group)])
                return carry

            lax.fori_loop(0, basis_pad // group, whole, 0)
            each(0, stack.columns, lambda step: stack.passing(step).start())

        edge = reduce_of(at.edge_reduce, FEAT, feat, lambda place: at.edge_send.at[place])
        at.edge_send[...] = at.edge_sum[...].astype(BF).reshape(feat, quarter, edges)
        each(0, edge.columns, lambda step: edge.passing(step).start())
        each(0, self_reduce.columns - 1, self_reduce.middle)
        ahead = min(1, stack.columns - 1)
        each(0, ahead, stack.middle)
        each(0, edge.columns - 1, edge.middle)

        at.scaled[...] = jnp.zeros((basis_rows, edges), F32)
        for chunk in range(chunks):
            lanes = pl.ds(chunk * span, span)
            grad = at.grad_message[:, lanes].astype(F32)
            for k in range(basis_count):
                value = at.products[k * quarter:(k + 1) * quarter, lanes].astype(F32) * grad
                at.scaled[k:k + 1, lanes] = jnp.sum(value, axis=0, keepdims=True)
        scaled = at.scaled[...]
        high = scaled.astype(BF)
        low = (scaled - high.astype(F32)).astype(BF)
        both = dot(jnp.concatenate([high, low], axis=0), at.rel_hot[...], 1, 1)
        coef_part = (both[:basis_rows] + both[basis_rows:]) * scale
        tall = jnp.concatenate(
            [coef_part[:, k * LANES:(k + 1) * LANES] for k in range(rel_pad // LANES)], axis=0
        )
        at.coef_out[...] = tall.reshape(dom, coef_rows, LANES)
        coef = Swap(
            DOM,
            dom,
            lambda place: at.coef_out.at[place],
            lambda place: at.coef_in.at[place],
            at.coef_sems,
        )
        coef.start()
        at.coef_in[me] = at.coef_out[me]
        each(ahead, stack.columns - 1, stack.middle)

        self_reduce.finish(at.self_sum)
        edge.finish(at.edge_total)
        at.edge_grad[...] = at.edge_total[...].astype(BF)
        node = reduce_of(at.node_reduce, DOM, dom, lambda place: at.nodes.at[place])

        def scatter(place):
            at.nodes[place] = dot(at.edge_grad[...], hot_of(place), 1, 1).astype(BF)

        def spread(step):
            place = node.place(step)
            scatter(place * 2 + 1 - node.side)
            node.passing(step).start()
            scatter(place * 2 + node.side)

        half = node.columns // 2
        each(0, half, spread)
        each(1, dom, lambda hop: coef.wait(hop))
        at.coef_feat[fme] = jnp.sum(at.coef_in[...], axis=0)
        coef_feat = Swap(
            FEAT,
            feat,
            lambda place: at.coef_feat.at[fme],
            lambda place: at.coef_feat.at[place],
            at.coef_feat_sems,
        )
        coef_feat.start()
        each(half, node.columns, spread)
        each(1, feat, lambda hop: coef_feat.wait(hop))
        coef_all_ref[me] = jnp.sum(at.coef_feat[...], axis=0)
        coef_all = Swap(
            DOM,
            dom,
            lambda place: coef_all_ref.at[me],
            lambda place: coef_all_ref.at[place],
            at.coef_all_sems,
        )
        coef_all.start()

        stack.finish(at.piece)
        pieces_ref[me] = (at.piece[...] * scale).astype(BF)
        pieces = Gather(
            DOM, dom, pieces_ref.at[me], lambda place: pieces_ref.at[place], at.pieces_sems
        )
        pieces.start()
        each(0, node.columns - 1, node.middle)
        each(1, pieces.columns, lambda hop: pieces.forward(hop))
        node.finish(at.node_sum)
        grad_feats_ref[...] = (at.self_sum[...] + at.node_sum[...]).astype(BF)
        each(0, pieces.columns, lambda hop: pieces.from_mate(hop))
        each(1, dom, lambda hop: coef_all.wait(hop))

        for done in [table, slot, own, message, back, coef, coef_feat, coef_all, pieces] + gathers:
            done.finish()
        for done in [self_reduce, stack, edge, node]:
            done.drain()

    vmem = pl.BlockSpec(memory_space=pltpu.VMEM)
    smem = pl.BlockSpec(memory_space=pltpu.SMEM)
    output, grad_feats, pieces, coef_all = pl.pallas_call(
        kernel,
        out_shape=(
            jax.ShapeDtypeStruct((quarter, entities), BF),
            jax.ShapeDtypeStruct((quarter, entities), BF),
            jax.ShapeDtypeStruct((dom, height, width), BF),
            jax.ShapeDtypeStruct((dom, coef_rows, LANES), F32),
        ),
        in_specs=[vmem, vmem, pl.BlockSpec(memory_space=pl.ANY)] + [vmem] * 6 + [smem] * 2,
        out_specs=(vmem,) * 4,
        scratch_shapes=shapes,
        compiler_params=pltpu.CompilerParams(
            collective_id=0, has_side_effects=True, vmem_limit_bytes=60 * 1024 * 1024
        ),
    )(feats, weight_t, bases, coef_t, part, row, dst, rel, cotangent, owner, valid)

    step = group_of(basis_count)
    halves = rel_pad // LANES

    def last(output_in, feats_in, bases_in, self_in, coef_in, *outs):
        outs[2][...] = bases_in[...].astype(F32).reshape(step, quarter, width)

        @pl.when(pl.program_id(0) == 0)
        def _():
            outs[0][...] = output_in[...]
            outs[1][...] = feats_in[...]
            outs[3][...] = self_in[...].astype(F32)
            parts = [coef_in[k * basis_rows:(k + 1) * basis_rows] for k in range(halves)]
            outs[4][...] = jnp.concatenate(parts, axis=1)[:basis_count, :relations]

    flat = pieces.reshape(total_rows, width)

    def fixed(shape, spot=0):
        return pl.BlockSpec(shape, lambda index: (spot,) + (0,) * (len(shape) - 1))

    output, grad_feats, grad_bases, grad_self, grad_coef = pl.pallas_call(
        last,
        grid=(basis_count // step,),
        out_shape=(
            jax.ShapeDtypeStruct((quarter, entities), BF),
            jax.ShapeDtypeStruct((quarter, entities), BF),
            jax.ShapeDtypeStruct((basis_count, quarter, width), F32),
            jax.ShapeDtypeStruct((quarter, width), F32),
            jax.ShapeDtypeStruct((basis_count, relations), F32),
        ),
        in_specs=[
            fixed((quarter, entities)),
            fixed((quarter, entities)),
            pl.BlockSpec((step * quarter, width), lambda index: (index, 0)),
            fixed((quarter, width), cut // quarter),
            fixed((halves * basis_rows, LANES)),
        ],
        out_specs=(
            fixed((quarter, entities)),
            fixed((quarter, entities)),
            pl.BlockSpec((step, quarter, width), lambda index: (index, 0, 0)),
            fixed((quarter, width)),
            fixed((basis_count, relations)),
        ),
    )(output, grad_feats, flat, flat, coef_all.reshape(halves * basis_rows, LANES))
    return output, grad_feats, grad_bases, grad_self.T, grad_coef.T


def body(
    feats,
    self_weight,
    bases,
    coef,
    src_part,
    src_row,
    edge_dst,
    edge_rel,
    block_owner,
    block_valid,
    cotangent,
):
    return layer(
        feats,
        self_weight.T,
        bases,
        coef.T,
        src_part.reshape(1, -1),
        src_row.reshape(1, -1),
        edge_dst.reshape(1, -1),
        edge_rel.reshape(1, -1),
        cotangent,
        block_owner.reshape(1, -1),
        block_valid,
        lax.axis_size(DOM),
        lax.axis_size(FEAT),
    )


def solution(mesh):
    return jax.shard_map(
        body,
        mesh=mesh,
        in_specs=(
            P(FEAT, DOM),
            P(None, FEAT),
            P(None, FEAT, None),
            P(),
            P(DOM, None),
            P(DOM),
            P(DOM),
            P(DOM),
            P(DOM, None),
            P(DOM, None),
            P(FEAT, DOM),
        ),
        out_specs=(P(FEAT, DOM), P(FEAT, DOM), P(None, FEAT, None), P(None, FEAT), P()),
        check_vma=False,
    )
```

```python
from types import SimpleNamespace

import jax
import jax.numpy as jnp
from jax import lax
from jax.experimental import pallas as pl
from jax.experimental.pallas import tpu as pltpu
from jax.sharding import PartitionSpec as P

BF = jnp.bfloat16
F32 = jnp.float32
I32 = jnp.int32
LANES = 128
ROUNDS = 1
PARTS = 2
NODE_AT = 4
DOM, FEAT = "dom", "feat"


def dot(left, right, left_axis, right_axis):
    return lax.dot_general(
        left, right, (((left_axis,), (right_axis,)), ((), ())), preferred_element_type=F32
    )


def first_of(ref):
    return lambda count: ref.at[pl.ds(0, count)]


def each(start, stop, step):
    if stop - start <= 8:
        for index in range(start, stop):
            step(index)
    else:
        lax.fori_loop(start, stop, lambda index, carry: (step(index), carry)[1], 0)


def peers(axis, count):
    me = lax.axis_index(axis)
    return me, me // 2, me % 2, count // 2


def greet(groups):
    barrier = pltpu.get_barrier_semaphore()
    for axis, count in groups:
        me = lax.axis_index(axis)

        def hello(hop):
            pl.semaphore_signal(
                barrier,
                inc=1,
                device_id={axis: (me + hop) % count},
                device_id_type=pl.DeviceIdType.MESH,
            )

        each(1, count, hello)
    return lambda: pl.semaphore_wait(barrier, sum(count - 1 for axis, count in groups))


def remote(source, target_ref, send_sem, recv_sem, axis, target):
    return pltpu.make_async_remote_copy(
        src_ref=source,
        dst_ref=target_ref,
        send_sem=send_sem,
        recv_sem=recv_sem,
        device_id={axis: target},
        device_id_type=pl.DeviceIdType.MESH,
    )


def wait_sent(region, sent, axis, target):
    remote(region, region, sent.at[0], sent.at[0], axis, target).wait_send()


class Gather:
    def __init__(self, axis, count, source, table, region, sems):
        self.me, self.spot, self.side, self.columns = peers(axis, count)
        self.axis, self.source, self.table, self.region = axis, source, table, region
        self.mate = self.spot * 2 + 1 - self.side
        self.sent, self.recvs, self.pair_recvs = sems

    def near(self, hop):
        step, top = hop - 1, self.columns - 1
        upper = self.spot // (self.columns // 2)
        up = step + (step - self.spot + self.columns) // self.columns
        mirrored = top - self.spot
        down = top - (step + (step - mirrored + self.columns) // self.columns)
        return up + upper * (down - up)

    def direct(self, hop):
        target = self.near(hop)
        return remote(
            self.source,
            self.table(self.me),
            self.sent.at[0],
            self.recvs.at[self.spot],
            self.axis,
            target * 2 + self.side,
        )

    def arrival(self, hop):
        spot = self.near(hop)
        block = self.table(spot * 2 + self.side)
        return remote(block, block, self.sent.at[0], self.recvs.at[spot], self.axis, self.mate)

    def place(self, hop, side):
        other = (hop + self.columns - 1) // self.columns
        return (self.spot + other * (self.near(hop) - self.spot)) * 2 + side

    def relay(self, hop, own=False):
        spot = self.table(self.place(hop, self.side))
        return remote(
            self.source if own else spot,
            spot,
            self.sent.at[0],
            self.pair_recvs.at[self.place(hop, 0) // 2],
            self.axis,
            self.mate,
        )

    def start(self):
        each(1, self.columns, lambda hop: self.direct(hop).start())
        self.relay(0, True).start()

    def forward(self, hop):
        self.arrival(hop).wait_recv()
        self.relay(hop).start()
        return self.place(hop, self.side)

    def from_mate(self, hop):
        self.relay(hop).wait_recv()
        return self.place(hop, 1 - self.side)

    def finish(self):
        wait_sent(self.region(2 * self.columns - 1), self.sent, self.axis, self.mate)


def gather_sems(count):
    columns = count // 2
    return [1, columns, columns]


class Swap:
    def __init__(self, axis, count, source, table, region, sems):
        self.me = lax.axis_index(axis)
        self.axis, self.count, self.source, self.table = axis, count, source, table
        self.region, self.together = region, sems[1].shape[0] == 1
        self.sent, self.recvs = sems

    def copy(self, hop):
        target = (self.me + hop) % self.count
        return remote(
            self.source(target),
            self.table(self.me),
            self.sent.at[0],
            self.recvs.at[0 if self.together else hop - 1],
            self.axis,
            target,
        )

    def start(self):
        each(1, self.count, lambda hop: self.copy(hop).start())

    def wait(self, hop):
        self.copy(hop).wait_recv()
        return (self.me - hop + self.count) % self.count

    def wait_all(self):
        region = self.region(self.count - 1)
        other = (self.me + 1) % self.count
        remote(region, region, self.sent.at[0], self.recvs.at[0], self.axis, other).wait_recv()

    def finish(self):
        other = (self.me + 1) % self.count
        wait_sent(self.region(self.count - 1), self.sent, self.axis, other)


def swap_sems(count, together=True):
    return [1, 1 if together else count - 1]


class Reduce:
    def __init__(self, axis, count, block, region, landed, summed, arrived, sems):
        self.me, self.spot, self.side, self.columns = peers(axis, count)
        self.axis, self.block, self.region = axis, block, region
        self.landed, self.summed, self.arrived = landed, summed, arrived
        self.sent, self.recvs, self.pair_recvs = sems

    def place(self, step):
        return (self.spot + 1 + step) % self.columns

    def passing(self, step):
        return remote(
            self.block(self.place(step) * 2 + 1 - self.side),
            self.landed.at[step],
            self.sent.at[0],
            self.pair_recvs.at[step],
            self.axis,
            self.spot * 2 + 1 - self.side,
        )

    def onward(self, step):
        return remote(
            self.summed.at[step],
            self.arrived.at[step],
            self.sent.at[0],
            self.recvs.at[step],
            self.axis,
            self.place(step) * 2 + self.side,
        )

    def pair(self, step):
        self.passing(step).wait_recv()
        own = self.block(self.place(step) * 2 + self.side)
        return own[...].astype(F32) + self.landed[step].astype(F32)

    def middle(self, step):
        self.summed[step] = self.pair(step).astype(BF)
        self.onward(step).start()

    def finish(self, total):
        total[...] = self.pair(self.columns - 1)

        def add(step):
            self.onward(step).wait_recv()
            total[...] += self.arrived[step].astype(F32)

        each(0, self.columns - 1, add)

    def drain(self):
        mate = self.spot * 2 + 1 - self.side
        wait_sent(self.region(2 * self.columns - 1), self.sent, self.axis, mate)


def sem_list(counts):
    return [pltpu.SemaphoreType.DMA((count,)) for count in counts]


def reduce_room(count, shape):
    columns = count // 2
    sizes = (columns, columns - 1, columns - 1)
    return [pltpu.VMEM((size,) + shape, BF) for size in sizes], sem_list(gather_sems(count))


def group_of(count):
    return max(size for size in range(1, 6) if count % size == 0)


def layer(
    feats, weight_t, bases, coef_t, part, row, dst, rel, cotangent, owner, valid, dom, feat
):
    quarter, entities = feats.shape
    width = weight_t.shape[1]
    edges = row.shape[1]
    blocks = valid.shape[1]
    rows = edges // blocks
    basis_count = bases.shape[0]
    relations = coef_t.shape[1]
    cap = max(1, 2 * blocks // dom)
    slots = cap * rows
    rel_pad = -(-relations // 256) * 256
    cut = basis_count * quarter
    total_rows = -(-(cut + quarter) // (16 * dom)) * 16 * dom
    while total_rows % quarter:
        total_rows += 16 * dom
    height = total_rows // dom
    basis_pad = total_rows // quarter
    rotated = height % quarter == 0
    group = height // quarter if rotated else group_of(basis_pad)
    rounds = ROUNDS if rotated and group % ROUNDS == 0 else 1
    bunch = group // rounds
    tall = height // rounds
    basis_rows = -(-basis_count // 8) * 8
    while basis_rows * rel_pad // LANES % dom:
        basis_rows += 8
    coef_rows = basis_rows * rel_pad // LANES // dom
    chunks = 2
    span = edges // chunks
    scale = float(edges * dom) ** (-0.5)

    room = SimpleNamespace()
    room.bases = pltpu.VMEM((basis_pad, quarter, width), BF)
    room.bases_sems = sem_list([1])
    room.weights = pltpu.VMEM((basis_pad, edges), F32)
    room.rel_hot = pltpu.VMEM((rel_pad, edges), BF)
    room.coef_wide = pltpu.VMEM((basis_rows, rel_pad), F32)
    room.sids = pltpu.VMEM((1, edges), I32)
    room.tids = pltpu.VMEM((blocks, 1, rows), I32)
    room.slot_out = pltpu.VMEM((dom, cap, rows), I32)
    room.slot_in = pltpu.VMEM((dom, cap, rows), I32)
    room.slot_sems = sem_list(swap_sems(dom))
    room.hots = pltpu.VMEM((dom, entities, slots), BF)
    room.degree = pltpu.VMEM((16, entities), F32)
    room.table = pltpu.VMEM((dom, quarter, entities), BF)
    room.table_sems = sem_list(gather_sems(dom))
    room.picked = pltpu.VMEM((quarter, edges), F32)
    room.own = pltpu.VMEM((feat, quarter, entities), BF)
    room.own_sems = sem_list(gather_sems(feat))
    room.sources = pltpu.VMEM((feat, quarter, edges), BF)
    room.source_sems = [sem_list(gather_sems(feat)) for chunk in range(chunks)]
    room.products = pltpu.VMEM((total_rows, edges), BF)
    room.messages = pltpu.VMEM((blocks, quarter, rows), BF)
    room.message_out = pltpu.VMEM((dom, cap, quarter, rows), BF)
    room.message_in = pltpu.VMEM((dom, cap, quarter, rows), BF)
    room.message_sems = sem_list(swap_sems(dom, False))
    room.preact = pltpu.VMEM((quarter, entities), F32)
    room.aggregate = pltpu.VMEM((quarter, entities), F32)
    room.grad_out = pltpu.VMEM((dom, cap, quarter, rows), BF)
    room.grad_in = pltpu.VMEM((dom * cap, quarter, rows), BF)
    room.grad_sems = sem_list(swap_sems(dom))
    room.grad_message = pltpu.VMEM((quarter, edges), BF)
    room.self_rows = pltpu.VMEM((quarter, width), BF)
    room.self_send = pltpu.VMEM((feat, quarter, entities), BF)
    room.self_reduce = reduce_room(feat, (quarter, entities))
    room.self_sum = pltpu.VMEM((quarter, entities), F32)
    room.stack = pltpu.VMEM((total_rows, width), BF)
    room.stack_reduce = [reduce_room(dom, (tall, width)) for part in range(rounds)]
    room.piece = pltpu.VMEM((height, width), F32)
    parts = PARTS if height % (16 * PARTS) == 0 else 1
    strip = height // parts
    room.pieces_sems = [sem_list(gather_sems(dom)) for part in range(parts)]
    room.scaled = pltpu.VMEM((basis_rows, edges), F32)
    room.combined = pltpu.VMEM((total_rows, edges), BF)
    room.edge_send = pltpu.VMEM((feat, quarter, edges), BF)
    room.edge_reduce = reduce_room(feat, (quarter, edges))
    room.edge_total = pltpu.VMEM((quarter, edges), F32)
    room.edge_grad = pltpu.VMEM((quarter, edges), BF)
    room.nodes = pltpu.VMEM((dom, quarter, entities), BF)
    room.node_reduce = reduce_room(dom, (quarter, entities))
    room.node_sum = pltpu.VMEM((quarter, entities), F32)
    room.coef_out = pltpu.VMEM((dom, coef_rows, LANES), F32)
    room.coef_in = pltpu.VMEM((dom, coef_rows, LANES), F32)
    room.coef_sems = sem_list(swap_sems(dom))
    room.coef_feat = pltpu.VMEM((feat, coef_rows, LANES), F32)
    room.coef_feat_sems = sem_list(swap_sems(feat))
    room.coef_all_sems = sem_list(swap_sems(dom))

    shapes, tree = jax.tree.flatten(vars(room))

    def kernel(
        feats_ref,
        weight_ref,
        bases_hbm,
        coef_ref,
        part_ref,
        row_ref,
        dst_ref,
        rel_ref,
        cot_ref,
        owner_ref,
        valid_ref,
        output_ref,
        grad_feats_ref,
        pieces_ref,
        coef_all_ref,
        *scratch,
    ):
        at = SimpleNamespace(**jax.tree.unflatten(tree, scratch))

        def reduce_of(space, axis, count, block, region):
            buffers, sems = space
            return Reduce(axis, count, block, region, *buffers, sems)

        me = lax.axis_index(DOM)
        fme = lax.axis_index(FEAT)
        met = greet([(DOM, dom), (FEAT, feat)])

        load = pltpu.make_async_copy(
            bases_hbm, at.bases.at[pl.ds(0, basis_count)], at.bases_sems[0].at[0]
        )
        load.start()
        if basis_pad > basis_count:
            extra = basis_pad - basis_count
            at.bases[basis_count:] = jnp.zeros((extra, quarter, width), BF)
        at.sids[...] = part_ref[...] * entities + row_ref[...]
        lane = lax.broadcasted_iota(I32, (1, rows), 1)
        spots = []
        for k in range(blocks):
            ids = dst_ref[:, k * rows:(k + 1) * rows]
            at.tids[k] = jnp.where(lane < valid_ref[0, k], ids, -1)
            rank = 0
            for other in range(k):
                rank = rank + jnp.where(owner_ref[0, other] == owner_ref[0, k], 1, 0)
            spots.append(owner_ref[0, k] * cap + rank)

        def block_at(slot):
            found = -1
            for k in range(blocks):
                found = jnp.where(spots[k] == slot, k, found)
            return found

        def fill(place):
            for j in range(cap):
                found = block_at(place * cap + j)
                used = jnp.where(found >= 0, 1, 0)
                ids = at.tids[jnp.maximum(found, 0)]
                at.slot_out[place, j:j + 1] = ids * used + (used - 1)

        each(0, dom, fill)
        at.slot_in[me] = at.slot_out[me]

        at.coef_wide[...] = jnp.zeros((basis_rows, rel_pad), F32)
        at.coef_wide[:basis_count, :relations] = coef_ref[...]
        wide = at.coef_wide[...]
        first = wide.astype(BF)
        second = (wide - first.astype(F32)).astype(BF)
        third = (wide - first.astype(F32) - second.astype(F32)).astype(BF)
        thirds = jnp.concatenate([first, second, third], axis=0)
        rel_rows = lax.broadcasted_iota(I32, (rel_pad, rows), 0)
        for k in range(blocks):
            lanes = slice(k * rows, (k + 1) * rows)
            at.rel_hot[:, lanes] = jnp.where(rel_rows == rel_ref[:, lanes], 1.0, 0.0).astype(BF)
        three = dot(thirds, at.rel_hot[...], 1, 0)
        weights = three[:basis_rows] + three[basis_rows:2 * basis_rows] + three[2 * basis_rows:]
        if basis_pad <= basis_rows:
            at.weights[...] = weights[:basis_pad]
        else:
            at.weights[:basis_rows] = weights
            at.weights[basis_rows:] = jnp.zeros((basis_pad - basis_rows, edges), F32)
        at.own[fme] = feats_ref[...]

        met()

        table = Gather(
            DOM, dom, feats_ref, lambda place: at.table.at[place], first_of(at.table), at.table_sems
        )
        slot = Swap(
            DOM,
            dom,
            lambda place: at.slot_out.at[place],
            lambda place: at.slot_in.at[place],
            first_of(at.slot_in),
            at.slot_sems,
        )
        slot.start()
        table.start()
        own = Gather(
            FEAT,
            feat,
            at.own.at[fme],
            lambda place: at.own.at[place],
            first_of(at.own),
            at.own_sems,
        )
        own.start()

        entity_rows = lax.broadcasted_iota(I32, (entities, edges), 0)

        def hot_of(place):
            hot = entity_rows + place * entities == at.sids[...]
            return jnp.where(hot, 1.0, 0.0).astype(BF)

        def use(place):
            at.picked[...] += dot(at.table[place], hot_of(place), 1, 0)

        at.picked[...] = dot(feats_ref[...], hot_of(me), 1, 0)
        use(table.from_mate(0))
        each(1, own.columns, lambda hop: own.forward(hop))
        each(1, table.columns, lambda hop: use(table.forward(hop)))
        each(1, table.columns, lambda hop: use(table.from_mate(hop)))

        gathers = []
        for chunk in range(chunks):
            lanes = pl.ds(chunk * span, span)
            at.sources[fme, :, lanes] = at.picked[:, lanes].astype(BF)
            gather = Gather(
                FEAT,
                feat,
                at.sources.at[fme, :, lanes],
                lambda place, lanes=lanes: at.sources.at[place, :, lanes],
                lambda count, lanes=lanes: at.sources.at[pl.ds(0, count), :, lanes],
                at.source_sems[chunk],
            )
            gather.start()
            gathers.append(gather)
        each(0, own.columns, lambda hop: own.from_mate(hop))
        own_full = at.own[...].reshape(width, entities)
        at.preact[...] = dot(weight_ref[...], own_full, 1, 0)
        load.wait()

        def forward(chunk):
            lanes = pl.ds(chunk * span, span)
            sources = at.sources[:, :, lanes].reshape(width, span)
            products = dot(at.bases[...].reshape(total_rows, width), sources, 1, 0)
            at.products[:, lanes] = products.astype(BF)
            total = jnp.zeros((quarter, span), F32)
            for k in range(basis_count):
                total += products[k * quarter:(k + 1) * quarter] * at.weights[k:k + 1, lanes]
            total = total.astype(BF)
            for k in range(span // rows):
                at.messages[chunk * (span // rows) + k] = total[:, k * rows:(k + 1) * rows]

        for gather in gathers:
            each(1, gather.columns, lambda hop: gather.forward(hop))
        for chunk, gather in enumerate(gathers):
            each(0, gather.columns, lambda hop: gather.from_mate(hop))
            forward(chunk)

        message = Swap(
            DOM,
            dom,
            lambda place: at.message_out.at[place],
            lambda place: at.message_in.at[place],
            first_of(at.message_in),
            at.message_sems,
        )

        def load_out(place):
            for j in range(cap):
                found = jnp.maximum(block_at(place * cap + j), 0)
                at.message_out[place, j] = at.messages[found]

        def send_out(hop):
            load_out((me + hop) % dom)
            message.copy(hop).start()

        each(1, dom, send_out)
        load_out(me)
        at.message_in[me] = at.message_out[me]

        slot_rows = lax.broadcasted_iota(I32, (entities, rows), 0)
        ones = jnp.ones((16, slots), BF)

        def slot_hot(place):
            parts = [
                jnp.where(slot_rows == at.slot_in[place, j:j + 1], 1.0, 0.0).astype(BF)
                for j in range(cap)
            ]
            hot = jnp.concatenate(parts, axis=1)
            at.hots[place] = hot
            at.degree[...] += dot(ones, hot, 1, 1)

        at.degree[...] = jnp.zeros((16, entities), F32)
        slot_hot(me)
        slot.wait_all()
        each(1, dom, lambda hop: slot_hot((me + hop) % dom))

        def gather_in(place):
            parts = [at.message_in[place, j] for j in range(cap)]
            value = jnp.concatenate(parts, axis=1)
            return dot(value, at.hots[place], 1, 1)

        at.aggregate[...] = gather_in(me)

        def take(hop):
            at.aggregate[...] += gather_in(message.wait(hop))

        each(1, dom, take)

        inverse = 1.0 / jnp.maximum(at.degree[0:1, :], 1.0)
        preact = at.preact[...] + inverse * at.aggregate[...]
        sigmoid = jax.nn.sigmoid(preact)
        output_ref[...] = (preact * sigmoid).astype(BF)
        grad_pre = (cot_ref[...].astype(F32) * sigmoid * (1.0 + preact * (1.0 - sigmoid))).astype(BF)
        grad_node = (grad_pre.astype(F32) * inverse).astype(BF)

        back = Swap(
            DOM,
            dom,
            lambda place: at.grad_out.at[place],
            lambda place: at.grad_in.at[pl.ds(place * cap, cap)],
            lambda count: at.grad_in.at[pl.ds(0, count * cap)],
            at.grad_sems,
        )

        def slot_grads(place, target):
            value = dot(grad_node, at.hots[place], 1, 0).astype(BF)
            for j in range(cap):
                target[j] = value[:, j * rows:(j + 1) * rows]

        def send_back(hop):
            place = (me + hop) % dom
            slot_grads(place, at.grad_out.at[place])
            back.copy(hop).start()

        each(1, dom, send_back)
        slot_grads(me, at.grad_in.at[pl.ds(me * cap, cap)])

        own_full = at.own[...].reshape(width, entities)
        at.self_rows[...] = dot(grad_pre, own_full, 1, 1).astype(BF)
        at.self_send[...] = (
            dot(weight_ref[...], grad_pre, 0, 0).astype(BF).reshape(feat, quarter, entities)
        )
        self_reduce = reduce_of(at.self_reduce, FEAT, feat, lambda place: at.self_send.at[place], first_of(at.self_send))
        each(0, self_reduce.columns, lambda step: self_reduce.passing(step).start())

        back.wait_all()
        for k in range(blocks):
            at.grad_message[:, k * rows:(k + 1) * rows] = at.grad_in[spots[k]]

        deep = bunch * quarter

        def combine(base):
            start = pl.multiple_of(base * quarter, deep)
            for chunk in range(chunks):
                lanes = pl.ds(chunk * span, span)
                grad = at.grad_message[:, lanes].astype(F32)
                for k in range(bunch):
                    weight = at.weights[pl.ds(base + k, 1), lanes]
                    spot = pl.ds(start + k * quarter, quarter)
                    at.combined[spot, lanes] = (grad * weight).astype(BF)
            block = at.combined[pl.ds(start, deep), :]
            piece = dot(block, at.sources[...].reshape(width, edges), 1, 1)
            at.stack[pl.ds(start, deep), :] = piece.astype(BF)

            @pl.when(base + bunch == basis_pad)
            def _():
                at.stack[cut:cut + quarter, :] = at.self_rows[...]

        def stack_of(part):
            def block(place):
                return at.stack.at[pl.ds(pl.multiple_of(place * height + part * tall, tall), tall)]

            def region(count):
                return at.stack.at[pl.ds(0, count * tall)]

            return reduce_of(at.stack_reduce[part], DOM, dom, block, region)

        stacks = [stack_of(part) for part in range(rounds)]
        last_step = stacks[0].columns - 1
        def coef_start():
            at.scaled[...] = jnp.zeros((basis_rows, edges), F32)
            for chunk in range(chunks):
                lanes = pl.ds(chunk * span, span)
                grad = at.grad_message[:, lanes].astype(F32)
                for k in range(basis_count):
                    value = at.products[k * quarter:(k + 1) * quarter, lanes].astype(F32) * grad
                    at.scaled[k:k + 1, lanes] = jnp.sum(value, axis=0, keepdims=True)
            scaled = at.scaled[...]
            high = scaled.astype(BF)
            low = (scaled - high.astype(F32)).astype(BF)
            both = dot(jnp.concatenate([high, low], axis=0), at.rel_hot[...], 1, 1)
            coef_part = (both[:basis_rows] + both[basis_rows:]) * scale
            stacked = jnp.concatenate(
                [coef_part[:, k * LANES:(k + 1) * LANES] for k in range(rel_pad // LANES)], axis=0
            )
            at.coef_out[...] = stacked.reshape(dom, coef_rows, LANES)
            coef = Swap(
                DOM,
                dom,
                lambda place: at.coef_out.at[place],
                lambda place: at.coef_in.at[place],
                first_of(at.coef_in),
            at.coef_sems,
            )
            coef.start()
            at.coef_in[me] = at.coef_out[me]
            return coef

        if rotated:

            def work(step):
                stack = stacks[part]
                place = stack.place(step)
                other = (place * 2 + 1 - stack.side) * group + part * bunch
                mine = (place * 2 + stack.side) * group + part * bunch
                combine(other)
                stack.passing(step).start()
                combine(mine)

            part = 0
            work(0)
            coef = coef_start()
            each(1, last_step + 1, work)
            for part in range(1, rounds):
                each(0, last_step + 1, work)
        else:

            def whole(index, carry):
                combine(index * bunch)
                return carry

            coef = coef_start()
            lax.fori_loop(0, basis_pad // bunch, whole, 0)
            each(0, last_step + 1, lambda step: stacks[0].passing(step).start())

        edge = reduce_of(at.edge_reduce, FEAT, feat, lambda place: at.edge_send.at[place], first_of(at.edge_send))
        every = at.bases[...].reshape(total_rows, width)
        edge_sum = dot(every, at.combined[...], 0, 0).astype(BF)
        at.edge_send[...] = edge_sum.reshape(feat, quarter, edges)
        each(0, edge.columns, lambda step: edge.passing(step).start())
        each(0, self_reduce.columns - 1, self_reduce.middle)
        soon = min(2, last_step)
        each(0, soon, stacks[0].middle)
        each(0, edge.columns - 1, edge.middle)
        each(soon, last_step, stacks[0].middle)

        coef.wait_all()
        at.coef_feat[fme] = jnp.sum(at.coef_in[...], axis=0)
        coef_feat = Swap(
            FEAT,
            feat,
            lambda place: at.coef_feat.at[fme],
            lambda place: at.coef_feat.at[place],
            first_of(at.coef_feat),
            at.coef_feat_sems,
        )
        coef_feat.start()
        for stack in stacks[1:]:
            each(0, soon, stack.middle)

        self_reduce.finish(at.self_sum)
        edge.finish(at.edge_total)
        at.edge_grad[...] = at.edge_total[...].astype(BF)
        node = reduce_of(at.node_reduce, DOM, dom, lambda place: at.nodes.at[place], first_of(at.nodes))

        def scatter(place):
            at.nodes[place] = dot(at.edge_grad[...], hot_of(place), 1, 1).astype(BF)

        def spread(step):
            place = node.place(step)
            scatter(place * 2 + 1 - node.side)
            node.passing(step).start()
            scatter(place * 2 + node.side)

        def piece_of(part):
            rows_of = pl.ds(part * strip, strip)
            return Gather(
                DOM,
                dom,
                pieces_ref.at[me, rows_of],
                lambda place: pieces_ref.at[place, rows_of],
                lambda count: pieces_ref.at[pl.ds(0, count), rows_of],
                at.pieces_sems[part],
            )

        pieces = [piece_of(part) for part in range(parts)]

        def piece_send(hop):
            for piece in pieces:
                piece.direct(hop).start()

        def piece_pass(hop):
            for piece in pieces:
                piece.forward(hop)

        for stack in stacks[1:]:
            each(soon, last_step, stack.middle)
        coef_feat.wait_all()
        coef_all_ref[me] = jnp.sum(at.coef_feat[...], axis=0)
        coef_all = Swap(
            DOM,
            dom,
            lambda place: coef_all_ref.at[me],
            lambda place: coef_all_ref.at[place],
            first_of(coef_all_ref),
            at.coef_all_sems,
        )
        coef_all.start()
        each(0, node.columns, spread)
        stacks[0].finish(at.piece)
        pieces_ref[me] = (at.piece[...] * scale).astype(BF)
        each(1, node.columns, piece_send)
        for piece in pieces:
            piece.relay(0, True).start()
        held = min(NODE_AT, node.columns)
        each(1, held, piece_pass)
        each(0, node.columns - 1, node.middle)
        each(held, node.columns, piece_pass)
        node.finish(at.node_sum)
        grad_feats_ref[...] = (at.self_sum[...] + at.node_sum[...]).astype(BF)
        for piece in pieces:
            each(0, piece.columns, lambda hop: piece.from_mate(hop))
        coef_all.wait_all()

        for done in [table, slot, own, message, back, coef, coef_feat, coef_all] + gathers + pieces:
            done.finish()
        for done in [self_reduce, edge, node] + stacks:
            done.drain()

    vmem = pl.BlockSpec(memory_space=pltpu.VMEM)
    smem = pl.BlockSpec(memory_space=pltpu.SMEM)
    output, grad_feats, pieces, coef_all = pl.pallas_call(
        kernel,
        out_shape=(
            jax.ShapeDtypeStruct((quarter, entities), BF),
            jax.ShapeDtypeStruct((quarter, entities), BF),
            jax.ShapeDtypeStruct((dom, height, width), BF),
            jax.ShapeDtypeStruct((dom, coef_rows, LANES), F32),
        ),
        in_specs=[vmem, vmem, pl.BlockSpec(memory_space=pl.ANY)] + [vmem] * 6 + [smem] * 2,
        out_specs=(vmem,) * 4,
        scratch_shapes=shapes,
        compiler_params=pltpu.CompilerParams(
            collective_id=0, has_side_effects=True, vmem_limit_bytes=60 * 1024 * 1024
        ),
    )(feats, weight_t, bases, coef_t, part, row, dst, rel, cotangent, owner, valid)

    step = group_of(basis_count)
    halves = rel_pad // LANES

    def last(output_in, feats_in, flat_in, coef_in, *outs):
        output_out, feats_out, bases_out, self_out, coef_out, wide, sem = outs
        copies = []
        for index in range(basis_count // step):
            spots = pl.ds(index * step, step)
            value = flat_in[index * step * quarter:(index + 1) * step * quarter, :]
            wide[spots] = value.astype(F32).reshape(step, quarter, width)
            copy = pltpu.make_async_copy(wide.at[spots], bases_out.at[spots], sem.at[index])
            copy.start()
            copies.append(copy)
        output_out[...] = output_in[...]
        feats_out[...] = feats_in[...]
        self_out[...] = flat_in[cut:cut + quarter, :].astype(F32)
        parts = [coef_in[k * basis_rows:(k + 1) * basis_rows] for k in range(halves)]
        coef_out[...] = jnp.concatenate(parts, axis=1)[:basis_count, :relations]
        for copy in copies:
            copy.wait()

    output, grad_feats, grad_bases, grad_self, grad_coef = pl.pallas_call(
        last,
        out_shape=(
            jax.ShapeDtypeStruct((quarter, entities), BF),
            jax.ShapeDtypeStruct((quarter, entities), BF),
            jax.ShapeDtypeStruct((basis_count, quarter, width), F32),
            jax.ShapeDtypeStruct((quarter, width), F32),
            jax.ShapeDtypeStruct((basis_count, relations), F32),
        ),
        in_specs=[vmem] * 4,
        out_specs=(vmem, vmem, pl.BlockSpec(memory_space=pl.ANY), vmem, vmem),
        scratch_shapes=[
            pltpu.VMEM((basis_count, quarter, width), F32),
            pltpu.SemaphoreType.DMA((basis_count // step,)),
        ],
    )(
        output,
        grad_feats,
        pieces.reshape(total_rows, width),
        coef_all.reshape(halves * basis_rows, LANES),
    )
    return output, grad_feats, grad_bases, grad_self.T, grad_coef.T


def body(
    feats,
    self_weight,
    bases,
    coef,
    src_part,
    src_row,
    edge_dst,
    edge_rel,
    block_owner,
    block_valid,
    cotangent,
):
    return layer(
        feats,
        self_weight.T,
        bases,
        coef.T,
        src_part.reshape(1, -1),
        src_row.reshape(1, -1),
        edge_dst.reshape(1, -1),
        edge_rel.reshape(1, -1),
        cotangent,
        block_owner.reshape(1, -1),
        block_valid,
        lax.axis_size(DOM),
        lax.axis_size(FEAT),
    )


def solution(mesh):
    return jax.shard_map(
        body,
        mesh=mesh,
        in_specs=(
            P(FEAT, DOM),
            P(None, FEAT),
            P(None, FEAT, None),
            P(),
            P(DOM, None),
            P(DOM),
            P(DOM),
            P(DOM),
            P(DOM, None),
            P(DOM, None),
            P(FEAT, DOM),
        ),
        out_specs=(P(FEAT, DOM), P(FEAT, DOM), P(None, FEAT, None), P(None, FEAT), P()),
        check_vma=False,
    )
```

```python
from types import SimpleNamespace

import jax
import jax.numpy as jnp
from jax import lax
from jax.experimental import pallas as pl
from jax.experimental.pallas import tpu as pltpu
from jax.sharding import PartitionSpec as P

BF = jnp.bfloat16
F32 = jnp.float32
I32 = jnp.int32
LANES = 128
ROUNDS = 1
PARTS = 4
DOM, FEAT = "dom", "feat"


def dot(left, right, left_axis, right_axis):
    return lax.dot_general(
        left, right, (((left_axis,), (right_axis,)), ((), ())), preferred_element_type=F32
    )


def first_of(ref):
    return lambda count: ref.at[pl.ds(0, count)]


def each(start, stop, step):
    if stop - start <= 8:
        for index in range(start, stop):
            step(index)
    else:
        lax.fori_loop(start, stop, lambda index, carry: (step(index), carry)[1], 0)


def peers(axis, count):
    me = lax.axis_index(axis)
    return me, me // 2, me % 2, count // 2


def greet(groups):
    barrier = pltpu.get_barrier_semaphore()
    for axis, count in groups:
        me = lax.axis_index(axis)

        def hello(hop):
            pl.semaphore_signal(
                barrier,
                inc=1,
                device_id={axis: (me + hop) % count},
                device_id_type=pl.DeviceIdType.MESH,
            )

        each(1, count, hello)
    return lambda: pl.semaphore_wait(barrier, sum(count - 1 for axis, count in groups))


def remote(source, target_ref, send_sem, recv_sem, axis, target):
    return pltpu.make_async_remote_copy(
        src_ref=source,
        dst_ref=target_ref,
        send_sem=send_sem,
        recv_sem=recv_sem,
        device_id={axis: target},
        device_id_type=pl.DeviceIdType.MESH,
    )


def wait_sent(region, sent, axis, target):
    remote(region, region, sent.at[0], sent.at[0], axis, target).wait_send()


class Gather:
    def __init__(self, axis, count, source, table, region, sems):
        self.me, self.spot, self.side, self.columns = peers(axis, count)
        self.axis, self.source, self.table, self.region = axis, source, table, region
        self.mate = self.spot * 2 + 1 - self.side
        self.sent, self.recvs, self.pair_recvs = sems

    def near(self, hop):
        step, top = hop - 1, self.columns - 1
        upper = self.spot // (self.columns // 2)
        up = step + (step - self.spot + self.columns) // self.columns
        mirrored = top - self.spot
        down = top - (step + (step - mirrored + self.columns) // self.columns)
        return up + upper * (down - up)

    def direct(self, hop):
        target = self.near(hop)
        return remote(
            self.source,
            self.table(self.me),
            self.sent.at[0],
            self.recvs.at[self.spot],
            self.axis,
            target * 2 + self.side,
        )

    def arrival(self, hop):
        spot = self.near(hop)
        block = self.table(spot * 2 + self.side)
        return remote(block, block, self.sent.at[0], self.recvs.at[spot], self.axis, self.mate)

    def place(self, hop, side):
        other = (hop + self.columns - 1) // self.columns
        return (self.spot + other * (self.near(hop) - self.spot)) * 2 + side

    def relay(self, hop, own=False):
        spot = self.table(self.place(hop, self.side))
        return remote(
            self.source if own else spot,
            spot,
            self.sent.at[0],
            self.pair_recvs.at[self.place(hop, 0) // 2],
            self.axis,
            self.mate,
        )

    def start(self):
        each(1, self.columns, lambda hop: self.direct(hop).start())
        self.relay(0, True).start()

    def forward(self, hop):
        self.arrival(hop).wait_recv()
        self.relay(hop).start()
        return self.place(hop, self.side)

    def from_mate(self, hop):
        self.relay(hop).wait_recv()
        return self.place(hop, 1 - self.side)

    def finish(self):
        wait_sent(self.region(2 * self.columns - 1), self.sent, self.axis, self.mate)


def gather_sems(count):
    columns = count // 2
    return [1, columns, columns]


class Chain:
    def __init__(self, axis, count, table, region, sems):
        self.me, self.spot, self.side, self.columns = peers(axis, count)
        self.axis, self.table, self.region = axis, table, region
        self.mate = self.spot * 2 + 1 - self.side
        self.sent, self.moved, self.recvs, self.pair_recvs = sems

    def step(self, spot, way):
        block = self.table(spot * 2 + self.side)
        upper = (way + 1) // 2
        return remote(
            block,
            block,
            self.moved.at[upper * self.columns + spot],
            self.recvs.at[spot],
            self.axis,
            (self.spot + way) * 2 + self.side,
        )

    def relay(self, spot, side):
        block = self.table(spot * 2 + side)
        return remote(
            block, block, self.sent.at[0], self.pair_recvs.at[spot], self.axis, self.mate
        )

    def can(self, way):
        return self.spot < self.columns - 1 if way > 0 else self.spot > 0

    def start(self):
        for way in (1, -1):

            @pl.when(self.can(way))
            def _():
                self.step(self.spot, way).start()

        self.relay(self.spot, self.side).start()

    def holds(self, spot):
        return jnp.logical_and(spot >= 0, spot < self.columns)

    def forward(self, hop):
        for way in (1, -1):
            spot = self.spot - way * hop

            @pl.when(self.holds(spot))
            def _():
                copy = self.step(spot, way)
                copy.wait_recv()

                @pl.when(self.can(way))
                def _():
                    copy.start()

                self.relay(spot, self.side).start()

    def from_mate(self, spot):
        self.relay(spot, 1 - self.side).wait_recv()

    def finish(self):
        wait_sent(self.region(self.columns), self.sent, self.axis, self.mate)

        def drain(hop):
            for way in (1, -1):
                spot = self.spot - way * hop

                @pl.when(jnp.logical_and(self.holds(spot), self.can(way)))
                def _():
                    self.step(spot, way).wait_send()

        each(0, self.columns, drain)


def chain_sems(count):
    columns = count // 2
    return [1, 2 * columns, columns, columns]


class Swap:
    def __init__(self, axis, count, source, table, region, sems):
        self.me = lax.axis_index(axis)
        self.axis, self.count, self.source, self.table = axis, count, source, table
        self.region, self.together = region, sems[1].shape[0] == 1
        self.sent, self.recvs = sems

    def copy(self, hop):
        target = (self.me + hop) % self.count
        return remote(
            self.source(target),
            self.table(self.me),
            self.sent.at[0],
            self.recvs.at[0 if self.together else hop - 1],
            self.axis,
            target,
        )

    def start(self):
        each(1, self.count, lambda hop: self.copy(hop).start())

    def wait(self, hop):
        self.copy(hop).wait_recv()
        return (self.me - hop + self.count) % self.count

    def wait_all(self):
        region = self.region(self.count - 1)
        other = (self.me + 1) % self.count
        remote(region, region, self.sent.at[0], self.recvs.at[0], self.axis, other).wait_recv()

    def finish(self):
        other = (self.me + 1) % self.count
        wait_sent(self.region(self.count - 1), self.sent, self.axis, other)


def swap_sems(count, together=True):
    return [1, 1 if together else count - 1]


class Reduce:
    def __init__(self, axis, count, block, region, landed, summed, arrived, sems):
        self.me, self.spot, self.side, self.columns = peers(axis, count)
        self.axis, self.block, self.region = axis, block, region
        self.landed, self.summed, self.arrived = landed, summed, arrived
        self.sent, self.recvs, self.pair_recvs = sems

    def place(self, step):
        return (self.spot + 1 + step) % self.columns

    def passing(self, step):
        return remote(
            self.block(self.place(step) * 2 + 1 - self.side),
            self.landed.at[step],
            self.sent.at[0],
            self.pair_recvs.at[step],
            self.axis,
            self.spot * 2 + 1 - self.side,
        )

    def onward(self, step):
        return remote(
            self.summed.at[step],
            self.arrived.at[step],
            self.sent.at[0],
            self.recvs.at[step],
            self.axis,
            self.place(step) * 2 + self.side,
        )

    def pair(self, step):
        self.passing(step).wait_recv()
        own = self.block(self.place(step) * 2 + self.side)
        return own[...].astype(F32) + self.landed[step].astype(F32)

    def middle(self, step):
        self.summed[step] = self.pair(step).astype(BF)
        self.onward(step).start()

    def finish(self, total):
        total[...] = self.pair(self.columns - 1)

        def add(step):
            self.onward(step).wait_recv()
            total[...] += self.arrived[step].astype(F32)

        each(0, self.columns - 1, add)

    def drain(self):
        mate = self.spot * 2 + 1 - self.side
        wait_sent(self.region(2 * self.columns - 1), self.sent, self.axis, mate)


def sem_list(counts):
    return [pltpu.SemaphoreType.DMA((count,)) for count in counts]


def reduce_room(count, shape):
    columns = count // 2
    sizes = (columns, columns - 1, columns - 1)
    return [pltpu.VMEM((size,) + shape, BF) for size in sizes], sem_list(gather_sems(count))


def group_of(count):
    return max(size for size in range(1, 6) if count % size == 0)


def layer(
    feats, weight_t, bases, coef_t, part, row, dst, rel, cotangent, owner, valid, dom, feat
):
    quarter, entities = feats.shape
    width = weight_t.shape[1]
    edges = row.shape[1]
    blocks = valid.shape[1]
    rows = edges // blocks
    basis_count = bases.shape[0]
    relations = coef_t.shape[1]
    cap = max(1, 2 * blocks // dom)
    slots = cap * rows
    rel_pad = -(-relations // 256) * 256
    cut = basis_count * quarter
    total_rows = -(-(cut + quarter) // (16 * dom)) * 16 * dom
    while total_rows % quarter:
        total_rows += 16 * dom
    height = total_rows // dom
    basis_pad = total_rows // quarter
    rotated = height % quarter == 0
    group = height // quarter if rotated else group_of(basis_pad)
    rounds = ROUNDS if rotated and group % ROUNDS == 0 else 1
    bunch = group // rounds
    tall = height // rounds
    basis_rows = -(-basis_count // 8) * 8
    while basis_rows * rel_pad // LANES % dom:
        basis_rows += 8
    coef_rows = basis_rows * rel_pad // LANES // dom
    chunks = 2
    span = edges // chunks
    scale = float(edges * dom) ** (-0.5)

    room = SimpleNamespace()
    room.bases = pltpu.VMEM((basis_pad, quarter, width), BF)
    room.bases_sems = sem_list([1])
    room.weights = pltpu.VMEM((basis_pad, edges), F32)
    room.rel_hot = pltpu.VMEM((rel_pad, edges), BF)
    room.coef_wide = pltpu.VMEM((basis_rows, rel_pad), F32)
    room.sids = pltpu.VMEM((1, edges), I32)
    room.tids = pltpu.VMEM((blocks, 1, rows), I32)
    room.slot_out = pltpu.VMEM((dom, cap, rows), I32)
    room.slot_in = pltpu.VMEM((dom, cap, rows), I32)
    room.slot_sems = sem_list(swap_sems(dom))
    room.hots = pltpu.VMEM((dom, entities, slots), BF)
    room.degree = pltpu.VMEM((16, entities), F32)
    room.table = pltpu.VMEM((dom, quarter, entities), BF)
    room.table_sems = sem_list(gather_sems(dom))
    room.picked = pltpu.VMEM((quarter, edges), F32)
    room.own = pltpu.VMEM((feat, quarter, entities), BF)
    room.own_sems = sem_list(gather_sems(feat))
    room.sources = pltpu.VMEM((feat, quarter, edges), BF)
    room.source_sems = [sem_list(gather_sems(feat)) for chunk in range(chunks)]
    room.products = pltpu.VMEM((total_rows, edges), BF)
    room.messages = pltpu.VMEM((blocks, quarter, rows), BF)
    room.message_out = pltpu.VMEM((dom, cap, quarter, rows), BF)
    room.message_in = pltpu.VMEM((dom, cap, quarter, rows), BF)
    room.message_sems = sem_list(swap_sems(dom, False))
    room.preact = pltpu.VMEM((quarter, entities), F32)
    room.aggregate = pltpu.VMEM((quarter, entities), F32)
    room.grad_out = pltpu.VMEM((dom, cap, quarter, rows), BF)
    room.grad_in = pltpu.VMEM((dom * cap, quarter, rows), BF)
    room.grad_sems = sem_list(swap_sems(dom))
    room.grad_message = pltpu.VMEM((quarter, edges), BF)
    room.self_rows = pltpu.VMEM((quarter, width), BF)
    room.self_send = pltpu.VMEM((feat, quarter, entities), BF)
    room.self_reduce = reduce_room(feat, (quarter, entities))
    room.self_sum = pltpu.VMEM((quarter, entities), F32)
    room.stack = pltpu.VMEM((total_rows, width), BF)
    room.stack_reduce = [reduce_room(dom, (tall, width)) for part in range(rounds)]
    room.piece = pltpu.VMEM((height, width), F32)
    parts = PARTS if height % (16 * PARTS) == 0 else 1
    strip = height // parts
    room.pieces_sems = [sem_list(chain_sems(dom)) for part in range(parts)]
    room.scaled = pltpu.VMEM((basis_rows, edges), F32)
    room.combined = pltpu.VMEM((total_rows, edges), BF)
    room.edge_send = pltpu.VMEM((feat, quarter, edges), BF)
    room.edge_reduce = reduce_room(feat, (quarter, edges))
    room.edge_total = pltpu.VMEM((quarter, edges), F32)
    room.edge_grad = pltpu.VMEM((quarter, edges), BF)
    room.nodes = pltpu.VMEM((dom, quarter, entities), BF)
    room.node_reduce = reduce_room(dom, (quarter, entities))
    room.node_sum = pltpu.VMEM((quarter, entities), F32)
    room.coef_out = pltpu.VMEM((dom, coef_rows, LANES), F32)
    room.coef_in = pltpu.VMEM((dom, coef_rows, LANES), F32)
    room.coef_sems = sem_list(swap_sems(dom))
    room.coef_feat = pltpu.VMEM((feat, coef_rows, LANES), F32)
    room.coef_feat_sems = sem_list(swap_sems(feat))
    room.coef_all_sems = sem_list(swap_sems(dom))

    shapes, tree = jax.tree.flatten(vars(room))

    def kernel(
        feats_ref,
        weight_ref,
        bases_hbm,
        coef_ref,
        part_ref,
        row_ref,
        dst_ref,
        rel_ref,
        cot_ref,
        owner_ref,
        valid_ref,
        output_ref,
        grad_feats_ref,
        pieces_ref,
        coef_all_ref,
        *scratch,
    ):
        at = SimpleNamespace(**jax.tree.unflatten(tree, scratch))

        def reduce_of(space, axis, count, block, region):
            buffers, sems = space
            return Reduce(axis, count, block, region, *buffers, sems)

        me = lax.axis_index(DOM)
        fme = lax.axis_index(FEAT)
        met = greet([(DOM, dom), (FEAT, feat)])

        load = pltpu.make_async_copy(
            bases_hbm, at.bases.at[pl.ds(0, basis_count)], at.bases_sems[0].at[0]
        )
        load.start()
        if basis_pad > basis_count:
            extra = basis_pad - basis_count
            at.bases[basis_count:] = jnp.zeros((extra, quarter, width), BF)
        at.sids[...] = part_ref[...] * entities + row_ref[...]
        lane = lax.broadcasted_iota(I32, (1, rows), 1)
        spots = []
        for k in range(blocks):
            ids = dst_ref[:, k * rows:(k + 1) * rows]
            at.tids[k] = jnp.where(lane < valid_ref[0, k], ids, -1)
            rank = 0
            for other in range(k):
                rank = rank + jnp.where(owner_ref[0, other] == owner_ref[0, k], 1, 0)
            spots.append(owner_ref[0, k] * cap + rank)

        def block_at(slot):
            found = -1
            for k in range(blocks):
                found = jnp.where(spots[k] == slot, k, found)
            return found

        def fill(place):
            for j in range(cap):
                found = block_at(place * cap + j)
                used = jnp.where(found >= 0, 1, 0)
                ids = at.tids[jnp.maximum(found, 0)]
                at.slot_out[place, j:j + 1] = ids * used + (used - 1)

        each(0, dom, fill)
        at.slot_in[me] = at.slot_out[me]

        at.coef_wide[...] = jnp.zeros((basis_rows, rel_pad), F32)
        at.coef_wide[:basis_count, :relations] = coef_ref[...]
        wide = at.coef_wide[...]
        first = wide.astype(BF)
        second = (wide - first.astype(F32)).astype(BF)
        third = (wide - first.astype(F32) - second.astype(F32)).astype(BF)
        thirds = jnp.concatenate([first, second, third], axis=0)
        rel_rows = lax.broadcasted_iota(I32, (rel_pad, rows), 0)
        for k in range(blocks):
            lanes = slice(k * rows, (k + 1) * rows)
            at.rel_hot[:, lanes] = jnp.where(rel_rows == rel_ref[:, lanes], 1.0, 0.0).astype(BF)
        three = dot(thirds, at.rel_hot[...], 1, 0)
        weights = three[:basis_rows] + three[basis_rows:2 * basis_rows] + three[2 * basis_rows:]
        if basis_pad <= basis_rows:
            at.weights[...] = weights[:basis_pad]
        else:
            at.weights[:basis_rows] = weights
            at.weights[basis_rows:] = jnp.zeros((basis_pad - basis_rows, edges), F32)
        at.own[fme] = feats_ref[...]

        met()

        table = Gather(
            DOM, dom, feats_ref, lambda place: at.table.at[place], first_of(at.table), at.table_sems
        )
        slot = Swap(
            DOM,
            dom,
            lambda place: at.slot_out.at[place],
            lambda place: at.slot_in.at[place],
            first_of(at.slot_in),
            at.slot_sems,
        )
        slot.start()
        table.start()
        own = Gather(
            FEAT,
            feat,
            at.own.at[fme],
            lambda place: at.own.at[place],
            first_of(at.own),
            at.own_sems,
        )
        own.start()

        entity_rows = lax.broadcasted_iota(I32, (entities, edges), 0)

        def hot_of(place):
            hot = entity_rows + place * entities == at.sids[...]
            return jnp.where(hot, 1.0, 0.0).astype(BF)

        def use(place):
            at.picked[...] += dot(at.table[place], hot_of(place), 1, 0)

        at.picked[...] = dot(feats_ref[...], hot_of(me), 1, 0)
        use(table.from_mate(0))
        each(1, own.columns, lambda hop: own.forward(hop))
        each(1, table.columns, lambda hop: use(table.forward(hop)))
        each(1, table.columns, lambda hop: use(table.from_mate(hop)))

        gathers = []
        for chunk in range(chunks):
            lanes = pl.ds(chunk * span, span)
            at.sources[fme, :, lanes] = at.picked[:, lanes].astype(BF)
            gather = Gather(
                FEAT,
                feat,
                at.sources.at[fme, :, lanes],
                lambda place, lanes=lanes: at.sources.at[place, :, lanes],
                lambda count, lanes=lanes: at.sources.at[pl.ds(0, count), :, lanes],
                at.source_sems[chunk],
            )
            gather.start()
            gathers.append(gather)
        each(0, own.columns, lambda hop: own.from_mate(hop))
        own_full = at.own[...].reshape(width, entities)
        at.preact[...] = dot(weight_ref[...], own_full, 1, 0)
        load.wait()

        def forward(chunk):
            lanes = pl.ds(chunk * span, span)
            sources = at.sources[:, :, lanes].reshape(width, span)
            products = dot(at.bases[...].reshape(total_rows, width), sources, 1, 0)
            at.products[:, lanes] = products.astype(BF)
            total = jnp.zeros((quarter, span), F32)
            for k in range(basis_count):
                total += products[k * quarter:(k + 1) * quarter] * at.weights[k:k + 1, lanes]
            total = total.astype(BF)
            for k in range(span // rows):
                at.messages[chunk * (span // rows) + k] = total[:, k * rows:(k + 1) * rows]

        for gather in gathers:
            each(1, gather.columns, lambda hop: gather.forward(hop))
        for chunk, gather in enumerate(gathers):
            each(0, gather.columns, lambda hop: gather.from_mate(hop))
            forward(chunk)

        message = Swap(
            DOM,
            dom,
            lambda place: at.message_out.at[place],
            lambda place: at.message_in.at[place],
            first_of(at.message_in),
            at.message_sems,
        )

        def load_out(place):
            for j in range(cap):
                found = jnp.maximum(block_at(place * cap + j), 0)
                at.message_out[place, j] = at.messages[found]

        def send_out(hop):
            load_out((me + hop) % dom)
            message.copy(hop).start()

        each(1, dom, send_out)
        load_out(me)
        at.message_in[me] = at.message_out[me]

        slot_rows = lax.broadcasted_iota(I32, (entities, rows), 0)
        ones = jnp.ones((16, slots), BF)

        def slot_hot(place):
            parts = [
                jnp.where(slot_rows == at.slot_in[place, j:j + 1], 1.0, 0.0).astype(BF)
                for j in range(cap)
            ]
            hot = jnp.concatenate(parts, axis=1)
            at.hots[place] = hot
            at.degree[...] += dot(ones, hot, 1, 1)

        at.degree[...] = jnp.zeros((16, entities), F32)
        slot_hot(me)
        slot.wait_all()
        each(1, dom, lambda hop: slot_hot((me + hop) % dom))

        def gather_in(place):
            parts = [at.message_in[place, j] for j in range(cap)]
            value = jnp.concatenate(parts, axis=1)
            return dot(value, at.hots[place], 1, 1)

        at.aggregate[...] = gather_in(me)

        def take(hop):
            at.aggregate[...] += gather_in(message.wait(hop))

        each(1, dom, take)

        inverse = 1.0 / jnp.maximum(at.degree[0:1, :], 1.0)
        preact = at.preact[...] + inverse * at.aggregate[...]
        sigmoid = jax.nn.sigmoid(preact)
        output_ref[...] = (preact * sigmoid).astype(BF)
        grad_pre = (cot_ref[...].astype(F32) * sigmoid * (1.0 + preact * (1.0 - sigmoid))).astype(BF)
        grad_node = (grad_pre.astype(F32) * inverse).astype(BF)

        back = Swap(
            DOM,
            dom,
            lambda place: at.grad_out.at[place],
            lambda place: at.grad_in.at[pl.ds(place * cap, cap)],
            lambda count: at.grad_in.at[pl.ds(0, count * cap)],
            at.grad_sems,
        )

        def slot_grads(place, target):
            value = dot(grad_node, at.hots[place], 1, 0).astype(BF)
            for j in range(cap):
                target[j] = value[:, j * rows:(j + 1) * rows]

        def send_back(hop):
            place = (me + hop) % dom
            slot_grads(place, at.grad_out.at[place])
            back.copy(hop).start()

        each(1, dom, send_back)
        slot_grads(me, at.grad_in.at[pl.ds(me * cap, cap)])

        own_full = at.own[...].reshape(width, entities)
        at.self_rows[...] = dot(grad_pre, own_full, 1, 1).astype(BF)
        at.self_send[...] = (
            dot(weight_ref[...], grad_pre, 0, 0).astype(BF).reshape(feat, quarter, entities)
        )
        self_reduce = reduce_of(at.self_reduce, FEAT, feat, lambda place: at.self_send.at[place], first_of(at.self_send))
        each(0, self_reduce.columns, lambda step: self_reduce.passing(step).start())

        back.wait_all()
        for k in range(blocks):
            at.grad_message[:, k * rows:(k + 1) * rows] = at.grad_in[spots[k]]

        deep = bunch * quarter

        def combine(base):
            start = pl.multiple_of(base * quarter, deep)
            for chunk in range(chunks):
                lanes = pl.ds(chunk * span, span)
                grad = at.grad_message[:, lanes].astype(F32)
                for k in range(bunch):
                    weight = at.weights[pl.ds(base + k, 1), lanes]
                    spot = pl.ds(start + k * quarter, quarter)
                    at.combined[spot, lanes] = (grad * weight).astype(BF)
            block = at.combined[pl.ds(start, deep), :]
            piece = dot(block, at.sources[...].reshape(width, edges), 1, 1)
            at.stack[pl.ds(start, deep), :] = piece.astype(BF)

            @pl.when(base + bunch == basis_pad)
            def _():
                at.stack[cut:cut + quarter, :] = at.self_rows[...]

        def stack_of(part):
            def block(place):
                return at.stack.at[pl.ds(pl.multiple_of(place * height + part * tall, tall), tall)]

            def region(count):
                return at.stack.at[pl.ds(0, count * tall)]

            return reduce_of(at.stack_reduce[part], DOM, dom, block, region)

        stacks = [stack_of(part) for part in range(rounds)]
        last_step = stacks[0].columns - 1
        def coef_start():
            at.scaled[...] = jnp.zeros((basis_rows, edges), F32)
            for chunk in range(chunks):
                lanes = pl.ds(chunk * span, span)
                grad = at.grad_message[:, lanes].astype(F32)
                for k in range(basis_count):
                    value = at.products[k * quarter:(k + 1) * quarter, lanes].astype(F32) * grad
                    at.scaled[k:k + 1, lanes] = jnp.sum(value, axis=0, keepdims=True)
            scaled = at.scaled[...]
            high = scaled.astype(BF)
            low = (scaled - high.astype(F32)).astype(BF)
            both = dot(jnp.concatenate([high, low], axis=0), at.rel_hot[...], 1, 1)
            coef_part = (both[:basis_rows] + both[basis_rows:]) * scale
            stacked = jnp.concatenate(
                [coef_part[:, k * LANES:(k + 1) * LANES] for k in range(rel_pad // LANES)], axis=0
            )
            at.coef_out[...] = stacked.reshape(dom, coef_rows, LANES)
            coef = Swap(
                DOM,
                dom,
                lambda place: at.coef_out.at[place],
                lambda place: at.coef_in.at[place],
                first_of(at.coef_in),
            at.coef_sems,
            )
            coef.start()
            at.coef_in[me] = at.coef_out[me]
            return coef

        if rotated:

            def work(step):
                stack = stacks[part]
                place = stack.place(step)
                other = (place * 2 + 1 - stack.side) * group + part * bunch
                mine = (place * 2 + stack.side) * group + part * bunch
                combine(other)
                stack.passing(step).start()
                combine(mine)

            part = 0
            work(0)
            coef = coef_start()
            each(1, last_step + 1, work)
            for part in range(1, rounds):
                each(0, last_step + 1, work)
        else:

            def whole(index, carry):
                combine(index * bunch)
                return carry

            coef = coef_start()
            lax.fori_loop(0, basis_pad // bunch, whole, 0)
            each(0, last_step + 1, lambda step: stacks[0].passing(step).start())

        edge = reduce_of(at.edge_reduce, FEAT, feat, lambda place: at.edge_send.at[place], first_of(at.edge_send))
        every = at.bases[...].reshape(total_rows, width)
        edge_sum = dot(every, at.combined[...], 0, 0).astype(BF)
        at.edge_send[...] = edge_sum.reshape(feat, quarter, edges)
        each(0, edge.columns, lambda step: edge.passing(step).start())
        each(0, self_reduce.columns - 1, self_reduce.middle)
        soon = min(2, last_step)
        each(0, soon, stacks[0].middle)
        each(0, edge.columns - 1, edge.middle)
        each(soon, last_step, stacks[0].middle)

        coef.wait_all()
        at.coef_feat[fme] = jnp.sum(at.coef_in[...], axis=0)
        coef_feat = Swap(
            FEAT,
            feat,
            lambda place: at.coef_feat.at[fme],
            lambda place: at.coef_feat.at[place],
            first_of(at.coef_feat),
            at.coef_feat_sems,
        )
        coef_feat.start()
        for stack in stacks[1:]:
            each(0, soon, stack.middle)

        self_reduce.finish(at.self_sum)
        edge.finish(at.edge_total)
        at.edge_grad[...] = at.edge_total[...].astype(BF)
        node = reduce_of(at.node_reduce, DOM, dom, lambda place: at.nodes.at[place], first_of(at.nodes))

        def scatter(place):
            at.nodes[place] = dot(at.edge_grad[...], hot_of(place), 1, 1).astype(BF)

        def spread(step):
            place = node.place(step)
            scatter(place * 2 + 1 - node.side)
            node.passing(step).start()
            scatter(place * 2 + node.side)

        def piece_of(part):
            rows_of = pl.ds(part * strip, strip)
            return Chain(
                DOM,
                dom,
                lambda place: pieces_ref.at[place, rows_of],
                lambda count: pieces_ref.at[pl.ds(0, count), rows_of],
                at.pieces_sems[part],
            )

        pieces = [piece_of(part) for part in range(parts)]

        def piece_pass(hop):
            for piece in pieces:
                piece.forward(hop)

        for stack in stacks[1:]:
            each(soon, last_step, stack.middle)
        coef_feat.wait_all()
        coef_all_ref[me] = jnp.sum(at.coef_feat[...], axis=0)
        coef_all = Swap(
            DOM,
            dom,
            lambda place: coef_all_ref.at[me],
            lambda place: coef_all_ref.at[place],
            first_of(coef_all_ref),
            at.coef_all_sems,
        )
        coef_all.start()
        each(0, node.columns, spread)
        stacks[0].finish(at.piece)
        pieces_ref[me] = (at.piece[...] * scale).astype(BF)
        for piece in pieces:
            piece.start()
        each(1, node.columns, piece_pass)
        each(0, node.columns - 1, node.middle)
        node.finish(at.node_sum)
        grad_feats_ref[...] = (at.self_sum[...] + at.node_sum[...]).astype(BF)
        for piece in pieces:
            each(0, piece.columns, lambda hop: piece.from_mate(hop))
        coef_all.wait_all()

        for done in [table, slot, own, message, back, coef, coef_feat, coef_all] + gathers + pieces:
            done.finish()
        for done in [self_reduce, edge, node] + stacks:
            done.drain()

    vmem = pl.BlockSpec(memory_space=pltpu.VMEM)
    smem = pl.BlockSpec(memory_space=pltpu.SMEM)
    output, grad_feats, pieces, coef_all = pl.pallas_call(
        kernel,
        out_shape=(
            jax.ShapeDtypeStruct((quarter, entities), BF),
            jax.ShapeDtypeStruct((quarter, entities), BF),
            jax.ShapeDtypeStruct((dom, height, width), BF),
            jax.ShapeDtypeStruct((dom, coef_rows, LANES), F32),
        ),
        in_specs=[vmem, vmem, pl.BlockSpec(memory_space=pl.ANY)] + [vmem] * 6 + [smem] * 2,
        out_specs=(vmem,) * 4,
        scratch_shapes=shapes,
        compiler_params=pltpu.CompilerParams(
            collective_id=0, has_side_effects=True, vmem_limit_bytes=60 * 1024 * 1024
        ),
    )(feats, weight_t, bases, coef_t, part, row, dst, rel, cotangent, owner, valid)

    step = group_of(basis_count)
    halves = rel_pad // LANES

    def last(output_in, feats_in, flat_in, coef_in, *outs):
        output_out, feats_out, bases_out, self_out, coef_out, wide, sem = outs
        copies = []
        for index in range(basis_count // step):
            spots = pl.ds(index * step, step)
            value = flat_in[index * step * quarter:(index + 1) * step * quarter, :]
            wide[spots] = value.astype(F32).reshape(step, quarter, width)
            copy = pltpu.make_async_copy(wide.at[spots], bases_out.at[spots], sem.at[index])
            copy.start()
            copies.append(copy)
        output_out[...] = output_in[...]
        feats_out[...] = feats_in[...]
        self_out[...] = flat_in[cut:cut + quarter, :].astype(F32)
        parts = [coef_in[k * basis_rows:(k + 1) * basis_rows] for k in range(halves)]
        coef_out[...] = jnp.concatenate(parts, axis=1)[:basis_count, :relations]
        for copy in copies:
            copy.wait()

    output, grad_feats, grad_bases, grad_self, grad_coef = pl.pallas_call(
        last,
        out_shape=(
            jax.ShapeDtypeStruct((quarter, entities), BF),
            jax.ShapeDtypeStruct((quarter, entities), BF),
            jax.ShapeDtypeStruct((basis_count, quarter, width), F32),
            jax.ShapeDtypeStruct((quarter, width), F32),
            jax.ShapeDtypeStruct((basis_count, relations), F32),
        ),
        in_specs=[vmem] * 4,
        out_specs=(vmem, vmem, pl.BlockSpec(memory_space=pl.ANY), vmem, vmem),
        scratch_shapes=[
            pltpu.VMEM((basis_count, quarter, width), F32),
            pltpu.SemaphoreType.DMA((basis_count // step,)),
        ],
    )(
        output,
        grad_feats,
        pieces.reshape(total_rows, width),
        coef_all.reshape(halves * basis_rows, LANES),
    )
    return output, grad_feats, grad_bases, grad_self.T, grad_coef.T


def body(
    feats,
    self_weight,
    bases,
    coef,
    src_part,
    src_row,
    edge_dst,
    edge_rel,
    block_owner,
    block_valid,
    cotangent,
):
    return layer(
        feats,
        self_weight.T,
        bases,
        coef.T,
        src_part.reshape(1, -1),
        src_row.reshape(1, -1),
        edge_dst.reshape(1, -1),
        edge_rel.reshape(1, -1),
        cotangent,
        block_owner.reshape(1, -1),
        block_valid,
        lax.axis_size(DOM),
        lax.axis_size(FEAT),
    )


def solution(mesh):
    return jax.shard_map(
        body,
        mesh=mesh,
        in_specs=(
            P(FEAT, DOM),
            P(None, FEAT),
            P(None, FEAT, None),
            P(),
            P(DOM, None),
            P(DOM),
            P(DOM),
            P(DOM),
            P(DOM, None),
            P(DOM, None),
            P(FEAT, DOM),
        ),
        out_specs=(P(FEAT, DOM), P(FEAT, DOM), P(None, FEAT, None), P(None, FEAT), P()),
        check_vma=False,
    )
```

```python
from types import SimpleNamespace

import jax
import jax.numpy as jnp
from jax import lax
from jax.experimental import pallas as pl
from jax.experimental.pallas import tpu as pltpu
from jax.sharding import PartitionSpec as P

BF = jnp.bfloat16
F32 = jnp.float32
I32 = jnp.int32
LANES = 128
ROUNDS = 1
PARTS = 4
DOM, FEAT = "dom", "feat"


def dot(left, right, left_axis, right_axis):
    return lax.dot_general(
        left, right, (((left_axis,), (right_axis,)), ((), ())), preferred_element_type=F32
    )


def first_of(ref):
    return lambda count: ref.at[pl.ds(0, count)]


def each(start, stop, step):
    if stop - start <= 8:
        for index in range(start, stop):
            step(index)
    else:
        lax.fori_loop(start, stop, lambda index, carry: (step(index), carry)[1], 0)


def peers(axis, count):
    me = lax.axis_index(axis)
    return me, me // 2, me % 2, count // 2


def greet(groups):
    barrier = pltpu.get_barrier_semaphore()
    for axis, count in groups:
        me = lax.axis_index(axis)

        def hello(hop):
            pl.semaphore_signal(
                barrier,
                inc=1,
                device_id={axis: (me + hop) % count},
                device_id_type=pl.DeviceIdType.MESH,
            )

        each(1, count, hello)
    return lambda: pl.semaphore_wait(barrier, sum(count - 1 for axis, count in groups))


def remote(source, target_ref, send_sem, recv_sem, axis, target):
    return pltpu.make_async_remote_copy(
        src_ref=source,
        dst_ref=target_ref,
        send_sem=send_sem,
        recv_sem=recv_sem,
        device_id={axis: target},
        device_id_type=pl.DeviceIdType.MESH,
    )


def wait_sent(region, sent, axis, target):
    remote(region, region, sent.at[0], sent.at[0], axis, target).wait_send()


class Gather:
    def __init__(self, axis, count, source, table, region, sems):
        self.me, self.spot, self.side, self.columns = peers(axis, count)
        self.axis, self.source, self.table, self.region = axis, source, table, region
        self.mate = self.spot * 2 + 1 - self.side
        self.sent, self.recvs, self.pair_recvs = sems

    def near(self, hop):
        step, top = hop - 1, self.columns - 1
        upper = self.spot // (self.columns // 2)
        up = step + (step - self.spot + self.columns) // self.columns
        mirrored = top - self.spot
        down = top - (step + (step - mirrored + self.columns) // self.columns)
        return up + upper * (down - up)

    def direct(self, hop):
        target = self.near(hop)
        return remote(
            self.source,
            self.table(self.me),
            self.sent.at[0],
            self.recvs.at[self.spot],
            self.axis,
            target * 2 + self.side,
        )

    def arrival(self, hop):
        spot = self.near(hop)
        block = self.table(spot * 2 + self.side)
        return remote(block, block, self.sent.at[0], self.recvs.at[spot], self.axis, self.mate)

    def place(self, hop, side):
        other = (hop + self.columns - 1) // self.columns
        return (self.spot + other * (self.near(hop) - self.spot)) * 2 + side

    def relay(self, hop, own=False):
        spot = self.table(self.place(hop, self.side))
        return remote(
            self.source if own else spot,
            spot,
            self.sent.at[0],
            self.pair_recvs.at[self.place(hop, 0) // 2],
            self.axis,
            self.mate,
        )

    def start(self):
        each(1, self.columns, lambda hop: self.direct(hop).start())
        self.relay(0, True).start()

    def forward(self, hop):
        self.arrival(hop).wait_recv()
        self.relay(hop).start()
        return self.place(hop, self.side)

    def from_mate(self, hop):
        self.relay(hop).wait_recv()
        return self.place(hop, 1 - self.side)

    def finish(self):
        wait_sent(self.region(2 * self.columns - 1), self.sent, self.axis, self.mate)


def gather_sems(count):
    columns = count // 2
    return [1, columns, columns]


class Chain:
    def __init__(self, axis, count, table, region, sems):
        self.me, self.spot, self.side, self.columns = peers(axis, count)
        self.axis, self.table, self.region = axis, table, region
        self.mate = self.spot * 2 + 1 - self.side
        self.sent, self.moved, self.recvs, self.pair_recvs = sems

    def step(self, spot, way):
        block = self.table(spot * 2 + self.side)
        upper = (way + 1) // 2
        return remote(
            block,
            block,
            self.moved.at[upper * self.columns + spot],
            self.recvs.at[spot],
            self.axis,
            (self.spot + way) * 2 + self.side,
        )

    def relay(self, spot, side):
        block = self.table(spot * 2 + side)
        return remote(
            block, block, self.sent.at[0], self.pair_recvs.at[spot], self.axis, self.mate
        )

    def can(self, way):
        return self.spot < self.columns - 1 if way > 0 else self.spot > 0

    def start(self):
        for way in (1, -1):

            @pl.when(self.can(way))
            def _():
                self.step(self.spot, way).start()

        self.relay(self.spot, self.side).start()

    def holds(self, spot):
        return jnp.logical_and(spot >= 0, spot < self.columns)

    def forward(self, hop):
        for way in (1, -1):
            spot = self.spot - way * hop

            @pl.when(self.holds(spot))
            def _():
                copy = self.step(spot, way)
                copy.wait_recv()

                @pl.when(self.can(way))
                def _():
                    copy.start()

                self.relay(spot, self.side).start()

    def from_mate(self, spot):
        self.relay(spot, 1 - self.side).wait_recv()

    def finish(self):
        wait_sent(self.region(self.columns), self.sent, self.axis, self.mate)

        def drain(hop):
            for way in (1, -1):
                spot = self.spot - way * hop

                @pl.when(jnp.logical_and(self.holds(spot), self.can(way)))
                def _():
                    self.step(spot, way).wait_send()

        each(0, self.columns, drain)


def chain_sems(count):
    columns = count // 2
    return [1, 2 * columns, columns, columns]


class Swap:
    def __init__(self, axis, count, source, table, region, sems):
        self.me = lax.axis_index(axis)
        self.axis, self.count, self.source, self.table = axis, count, source, table
        self.region, self.together = region, sems[1].shape[0] == 1
        self.sent, self.recvs = sems

    def copy(self, hop):
        target = (self.me + hop) % self.count
        return remote(
            self.source(target),
            self.table(self.me),
            self.sent.at[0],
            self.recvs.at[0 if self.together else hop - 1],
            self.axis,
            target,
        )

    def start(self):
        each(1, self.count, lambda hop: self.copy(hop).start())

    def wait(self, hop):
        self.copy(hop).wait_recv()
        return (self.me - hop + self.count) % self.count

    def wait_all(self):
        region = self.region(self.count - 1)
        other = (self.me + 1) % self.count
        remote(region, region, self.sent.at[0], self.recvs.at[0], self.axis, other).wait_recv()

    def finish(self):
        other = (self.me + 1) % self.count
        wait_sent(self.region(self.count - 1), self.sent, self.axis, other)


def swap_sems(count, together=True):
    return [1, 1 if together else count - 1]


class Reduce:
    def __init__(self, axis, count, block, region, landed, summed, arrived, sems):
        self.me, self.spot, self.side, self.columns = peers(axis, count)
        self.axis, self.block, self.region = axis, block, region
        self.landed, self.summed, self.arrived = landed, summed, arrived
        self.sent, self.recvs, self.pair_recvs = sems

    def place(self, step):
        return (self.spot + 1 + step) % self.columns

    def passing(self, step):
        return remote(
            self.block(self.place(step) * 2 + 1 - self.side),
            self.landed.at[step],
            self.sent.at[0],
            self.pair_recvs.at[step],
            self.axis,
            self.spot * 2 + 1 - self.side,
        )

    def onward(self, step):
        return remote(
            self.summed.at[step],
            self.arrived.at[step],
            self.sent.at[0],
            self.recvs.at[step],
            self.axis,
            self.place(step) * 2 + self.side,
        )

    def pair(self, step):
        self.passing(step).wait_recv()
        own = self.block(self.place(step) * 2 + self.side)
        return own[...].astype(F32) + self.landed[step].astype(F32)

    def middle(self, step):
        self.summed[step] = self.pair(step).astype(BF)
        self.onward(step).start()

    def finish(self, total):
        total[...] = self.pair(self.columns - 1)

        def add(step):
            self.onward(step).wait_recv()
            total[...] += self.arrived[step].astype(F32)

        each(0, self.columns - 1, add)

    def drain(self):
        mate = self.spot * 2 + 1 - self.side
        wait_sent(self.region(2 * self.columns - 1), self.sent, self.axis, mate)


def sem_list(counts):
    return [pltpu.SemaphoreType.DMA((count,)) for count in counts]


def reduce_room(count, shape):
    columns = count // 2
    sizes = (columns, columns - 1, columns - 1)
    return [pltpu.VMEM((size,) + shape, BF) for size in sizes], sem_list(gather_sems(count))


def group_of(count):
    return max(size for size in range(1, 6) if count % size == 0)


def layer(
    feats, weight_t, bases, coef_t, part, row, dst, rel, cotangent, owner, valid, dom, feat
):
    quarter, entities = feats.shape
    width = weight_t.shape[1]
    edges = row.shape[1]
    blocks = valid.shape[1]
    rows = edges // blocks
    basis_count = bases.shape[0]
    relations = coef_t.shape[1]
    cap = max(1, 2 * blocks // dom)
    slots = cap * rows
    rel_pad = -(-relations // 256) * 256
    cut = basis_count * quarter
    total_rows = -(-(cut + quarter) // (16 * dom)) * 16 * dom
    while total_rows % quarter:
        total_rows += 16 * dom
    height = total_rows // dom
    basis_pad = total_rows // quarter
    rotated = height % quarter == 0
    group = height // quarter if rotated else group_of(basis_pad)
    rounds = ROUNDS if rotated and group % ROUNDS == 0 else 1
    bunch = group // rounds
    tall = height // rounds
    basis_rows = -(-basis_count // 8) * 8
    while basis_rows * rel_pad // LANES % dom:
        basis_rows += 8
    coef_rows = basis_rows * rel_pad // LANES // dom
    chunks = 2
    span = edges // chunks
    scale = float(edges * dom) ** (-0.5)

    room = SimpleNamespace()
    room.bases = pltpu.VMEM((basis_pad, quarter, width), BF)
    given = (feats, weight_t, coef_t, part, row, dst, rel, cotangent)
    room.given = [pltpu.VMEM(value.shape, value.dtype) for value in given]
    room.counts = [pltpu.SMEM(value.shape, value.dtype) for value in (owner, valid)]
    room.load_sems = sem_list([3 + len(given)])
    room.weights = pltpu.VMEM((basis_pad, edges), F32)
    room.rel_hot = pltpu.VMEM((rel_pad, edges), BF)
    room.coef_wide = pltpu.VMEM((basis_rows, rel_pad), F32)
    room.sids = pltpu.VMEM((1, edges), I32)
    room.tids = pltpu.VMEM((blocks, 1, rows), I32)
    room.slot_out = pltpu.VMEM((dom, cap, rows), I32)
    room.slot_in = pltpu.VMEM((dom, cap, rows), I32)
    room.slot_sems = sem_list(swap_sems(dom))
    room.hots = pltpu.VMEM((dom, entities, slots), BF)
    room.degree = pltpu.VMEM((16, entities), F32)
    room.table = pltpu.VMEM((dom, quarter, entities), BF)
    bands = 2 if quarter % 32 == 0 else 1
    band = quarter // bands
    room.table_sems = [sem_list(gather_sems(dom)) for part in range(bands)]
    room.picked = pltpu.VMEM((quarter, edges), F32)
    room.own = pltpu.VMEM((feat, quarter, entities), BF)
    room.own_sems = sem_list(gather_sems(feat))
    room.sources = pltpu.VMEM((feat, quarter, edges), BF)
    room.source_sems = [sem_list(gather_sems(feat)) for chunk in range(chunks)]
    room.products = pltpu.VMEM((total_rows, edges), BF)
    room.messages = pltpu.VMEM((blocks, quarter, rows), BF)
    room.message_out = pltpu.VMEM((dom, cap, quarter, rows), BF)
    room.message_in = pltpu.VMEM((dom, cap, quarter, rows), BF)
    room.message_sems = sem_list(swap_sems(dom, False))
    room.preact = pltpu.VMEM((quarter, entities), F32)
    room.aggregate = pltpu.VMEM((quarter, entities), F32)
    room.grad_out = pltpu.VMEM((dom, cap, quarter, rows), BF)
    room.grad_in = pltpu.VMEM((dom * cap, quarter, rows), BF)
    room.grad_sems = sem_list(swap_sems(dom))
    room.grad_message = pltpu.VMEM((quarter, edges), BF)
    room.self_rows = pltpu.VMEM((quarter, width), BF)
    room.self_send = pltpu.VMEM((feat, quarter, entities), BF)
    room.self_reduce = reduce_room(feat, (quarter, entities))
    room.self_sum = pltpu.VMEM((quarter, entities), F32)
    room.stack = pltpu.VMEM((total_rows, width), BF)
    room.stack_reduce = [reduce_room(dom, (tall, width)) for part in range(rounds)]
    room.piece = pltpu.VMEM((height, width), F32)
    parts = PARTS if height % (16 * PARTS) == 0 else 1
    strip = height // parts
    room.pieces_sems = [sem_list(chain_sems(dom)) for part in range(parts)]
    room.scaled = pltpu.VMEM((basis_rows, edges), F32)
    room.combined = pltpu.VMEM((total_rows, edges), BF)
    room.edge_send = pltpu.VMEM((feat, quarter, edges), BF)
    room.edge_reduce = reduce_room(feat, (quarter, edges))
    room.edge_total = pltpu.VMEM((quarter, edges), F32)
    room.edge_grad = pltpu.VMEM((quarter, edges), BF)
    room.nodes = pltpu.VMEM((dom, quarter, entities), BF)
    room.node_reduce = reduce_room(dom, (quarter, entities))
    room.node_sum = pltpu.VMEM((quarter, entities), F32)
    room.coef_out = pltpu.VMEM((dom, coef_rows, LANES), F32)
    room.coef_in = pltpu.VMEM((dom, coef_rows, LANES), F32)
    room.coef_sems = sem_list(swap_sems(dom))
    room.coef_feat = pltpu.VMEM((feat, coef_rows, LANES), F32)
    room.coef_feat_sems = sem_list(swap_sems(feat))
    room.coef_all_sems = sem_list(swap_sems(dom))

    shapes, tree = jax.tree.flatten(vars(room))

    def kernel(
        bases_hbm,
        feats_hbm,
        weight_hbm,
        coef_hbm,
        part_hbm,
        row_hbm,
        dst_hbm,
        rel_hbm,
        cot_hbm,
        owner_hbm,
        valid_hbm,
        output_ref,
        grad_feats_ref,
        pieces_ref,
        coef_all_ref,
        *scratch,
    ):
        at = SimpleNamespace(**jax.tree.unflatten(tree, scratch))

        def reduce_of(space, axis, count, block, region):
            buffers, sems = space
            return Reduce(axis, count, block, region, *buffers, sems)

        me = lax.axis_index(DOM)
        fme = lax.axis_index(FEAT)
        met = greet([(DOM, dom), (FEAT, feat)])

        feats_ref, weight_ref, coef_ref, part_ref, row_ref, dst_ref, rel_ref, cot_ref = at.given
        owner_ref, valid_ref = at.counts
        pairs = [
            (feats_hbm, feats_ref),
            (weight_hbm, weight_ref),
            (coef_hbm, coef_ref),
            (part_hbm, part_ref),
            (row_hbm, row_ref),
            (dst_hbm, dst_ref),
            (rel_hbm, rel_ref),
            (cot_hbm, cot_ref),
            (owner_hbm, owner_ref),
            (valid_hbm, valid_ref),
            (bases_hbm, at.bases.at[pl.ds(0, basis_count)]),
        ]
        loads = [
            pltpu.make_async_copy(source, target, at.load_sems[0].at[index])
            for index, (source, target) in enumerate(pairs)
        ]
        for load in loads:
            load.start()
        if basis_pad > basis_count:
            extra = basis_pad - basis_count
            at.bases[basis_count:] = jnp.zeros((extra, quarter, width), BF)
        for load in loads[:-1]:
            load.wait()
        at.sids[...] = part_ref[...] * entities + row_ref[...]
        lane = lax.broadcasted_iota(I32, (1, rows), 1)
        spots = []
        for k in range(blocks):
            ids = dst_ref[:, k * rows:(k + 1) * rows]
            at.tids[k] = jnp.where(lane < valid_ref[0, k], ids, -1)
            rank = 0
            for other in range(k):
                rank = rank + jnp.where(owner_ref[0, other] == owner_ref[0, k], 1, 0)
            spots.append(owner_ref[0, k] * cap + rank)

        def block_at(slot):
            found = -1
            for k in range(blocks):
                found = jnp.where(spots[k] == slot, k, found)
            return found

        def fill(place):
            for j in range(cap):
                found = block_at(place * cap + j)
                used = jnp.where(found >= 0, 1, 0)
                ids = at.tids[jnp.maximum(found, 0)]
                at.slot_out[place, j:j + 1] = ids * used + (used - 1)

        each(0, dom, fill)
        at.slot_in[me] = at.slot_out[me]

        at.coef_wide[...] = jnp.zeros((basis_rows, rel_pad), F32)
        at.coef_wide[:basis_count, :relations] = coef_ref[...]
        wide = at.coef_wide[...]
        first = wide.astype(BF)
        second = (wide - first.astype(F32)).astype(BF)
        third = (wide - first.astype(F32) - second.astype(F32)).astype(BF)
        thirds = jnp.concatenate([first, second, third], axis=0)
        rel_rows = lax.broadcasted_iota(I32, (rel_pad, rows), 0)
        for k in range(blocks):
            lanes = slice(k * rows, (k + 1) * rows)
            at.rel_hot[:, lanes] = jnp.where(rel_rows == rel_ref[:, lanes], 1.0, 0.0).astype(BF)
        three = dot(thirds, at.rel_hot[...], 1, 0)
        weights = three[:basis_rows] + three[basis_rows:2 * basis_rows] + three[2 * basis_rows:]
        if basis_pad <= basis_rows:
            at.weights[...] = weights[:basis_pad]
        else:
            at.weights[:basis_rows] = weights
            at.weights[basis_rows:] = jnp.zeros((basis_pad - basis_rows, edges), F32)
        at.own[fme] = feats_ref[...]

        met()

        def table_of(part):
            rows_of = pl.ds(part * band, band)
            return Gather(
                DOM,
                dom,
                feats_ref.at[rows_of],
                lambda place: at.table.at[place, rows_of],
                lambda count: at.table.at[pl.ds(0, count), rows_of],
                at.table_sems[part],
            )

        tables = [table_of(part) for part in range(bands)]

        def table_pass(hop):
            return [table.forward(hop) for table in tables][0]

        def table_take(hop):
            return [table.from_mate(hop) for table in tables][0]

        slot = Swap(
            DOM,
            dom,
            lambda place: at.slot_out.at[place],
            lambda place: at.slot_in.at[place],
            first_of(at.slot_in),
            at.slot_sems,
        )
        slot.start()
        each(1, tables[0].columns, lambda hop: [table.direct(hop).start() for table in tables])
        for table in tables:
            table.relay(0, True).start()
        own = Gather(
            FEAT,
            feat,
            at.own.at[fme],
            lambda place: at.own.at[place],
            first_of(at.own),
            at.own_sems,
        )
        own.start()

        entity_rows = lax.broadcasted_iota(I32, (entities, edges), 0)

        def hot_of(place):
            hot = entity_rows + place * entities == at.sids[...]
            return jnp.where(hot, 1.0, 0.0).astype(BF)

        def use(place):
            at.picked[...] += dot(at.table[place], hot_of(place), 1, 0)

        at.picked[...] = dot(feats_ref[...], hot_of(me), 1, 0)
        use(table_take(0))
        each(1, own.columns, lambda hop: own.forward(hop))
        each(1, tables[0].columns, lambda hop: use(table_pass(hop)))
        each(1, tables[0].columns, lambda hop: use(table_take(hop)))

        gathers = []
        for chunk in range(chunks):
            lanes = pl.ds(chunk * span, span)
            at.sources[fme, :, lanes] = at.picked[:, lanes].astype(BF)
            gather = Gather(
                FEAT,
                feat,
                at.sources.at[fme, :, lanes],
                lambda place, lanes=lanes: at.sources.at[place, :, lanes],
                lambda count, lanes=lanes: at.sources.at[pl.ds(0, count), :, lanes],
                at.source_sems[chunk],
            )
            gather.start()
            gathers.append(gather)
        each(0, own.columns, lambda hop: own.from_mate(hop))
        own_full = at.own[...].reshape(width, entities)
        at.preact[...] = dot(weight_ref[...], own_full, 1, 0)
        loads[-1].wait()

        def forward(chunk):
            lanes = pl.ds(chunk * span, span)
            sources = at.sources[:, :, lanes].reshape(width, span)
            products = dot(at.bases[...].reshape(total_rows, width), sources, 1, 0)
            at.products[:, lanes] = products.astype(BF)
            total = jnp.zeros((quarter, span), F32)
            for k in range(basis_count):
                total += products[k * quarter:(k + 1) * quarter] * at.weights[k:k + 1, lanes]
            total = total.astype(BF)
            for k in range(span // rows):
                at.messages[chunk * (span // rows) + k] = total[:, k * rows:(k + 1) * rows]

        for gather in gathers:
            each(1, gather.columns, lambda hop: gather.forward(hop))
        for chunk, gather in enumerate(gathers):
            each(0, gather.columns, lambda hop: gather.from_mate(hop))
            forward(chunk)

        message = Swap(
            DOM,
            dom,
            lambda place: at.message_out.at[place],
            lambda place: at.message_in.at[place],
            first_of(at.message_in),
            at.message_sems,
        )

        def load_out(place):
            for j in range(cap):
                found = jnp.maximum(block_at(place * cap + j), 0)
                at.message_out[place, j] = at.messages[found]

        def send_out(hop):
            load_out((me + hop) % dom)
            message.copy(hop).start()

        each(1, dom, send_out)
        load_out(me)
        at.message_in[me] = at.message_out[me]

        slot_rows = lax.broadcasted_iota(I32, (entities, rows), 0)
        ones = jnp.ones((16, slots), BF)

        def slot_hot(place):
            parts = [
                jnp.where(slot_rows == at.slot_in[place, j:j + 1], 1.0, 0.0).astype(BF)
                for j in range(cap)
            ]
            hot = jnp.concatenate(parts, axis=1)
            at.hots[place] = hot
            at.degree[...] += dot(ones, hot, 1, 1)

        at.degree[...] = jnp.zeros((16, entities), F32)
        slot_hot(me)
        slot.wait_all()
        each(1, dom, lambda hop: slot_hot((me + hop) % dom))

        def gather_in(place):
            parts = [at.message_in[place, j] for j in range(cap)]
            value = jnp.concatenate(parts, axis=1)
            return dot(value, at.hots[place], 1, 1)

        at.aggregate[...] = gather_in(me)

        def take(hop):
            at.aggregate[...] += gather_in(message.wait(hop))

        each(1, dom, take)

        inverse = 1.0 / jnp.maximum(at.degree[0:1, :], 1.0)
        preact = at.preact[...] + inverse * at.aggregate[...]
        sigmoid = jax.nn.sigmoid(preact)
        output_ref[...] = (preact * sigmoid).astype(BF)
        grad_pre = (cot_ref[...].astype(F32) * sigmoid * (1.0 + preact * (1.0 - sigmoid))).astype(BF)
        grad_node = (grad_pre.astype(F32) * inverse).astype(BF)

        back = Swap(
            DOM,
            dom,
            lambda place: at.grad_out.at[place],
            lambda place: at.grad_in.at[pl.ds(place * cap, cap)],
            lambda count: at.grad_in.at[pl.ds(0, count * cap)],
            at.grad_sems,
        )

        def slot_grads(place, target):
            value = dot(grad_node, at.hots[place], 1, 0).astype(BF)
            for j in range(cap):
                target[j] = value[:, j * rows:(j + 1) * rows]

        def send_back(hop):
            place = (me + hop) % dom
            slot_grads(place, at.grad_out.at[place])
            back.copy(hop).start()

        each(1, dom, send_back)
        slot_grads(me, at.grad_in.at[pl.ds(me * cap, cap)])

        own_full = at.own[...].reshape(width, entities)
        at.self_rows[...] = dot(grad_pre, own_full, 1, 1).astype(BF)
        at.self_send[...] = (
            dot(weight_ref[...], grad_pre, 0, 0).astype(BF).reshape(feat, quarter, entities)
        )
        self_reduce = reduce_of(at.self_reduce, FEAT, feat, lambda place: at.self_send.at[place], first_of(at.self_send))
        each(0, self_reduce.columns, lambda step: self_reduce.passing(step).start())

        back.wait_all()
        for k in range(blocks):
            at.grad_message[:, k * rows:(k + 1) * rows] = at.grad_in[spots[k]]

        deep = bunch * quarter

        def combine(base):
            start = pl.multiple_of(base * quarter, deep)
            for chunk in range(chunks):
                lanes = pl.ds(chunk * span, span)
                grad = at.grad_message[:, lanes].astype(F32)
                for k in range(bunch):
                    weight = at.weights[pl.ds(base + k, 1), lanes]
                    spot = pl.ds(start + k * quarter, quarter)
                    at.combined[spot, lanes] = (grad * weight).astype(BF)
            block = at.combined[pl.ds(start, deep), :]
            piece = dot(block, at.sources[...].reshape(width, edges), 1, 1)
            at.stack[pl.ds(start, deep), :] = piece.astype(BF)

            @pl.when(base + bunch == basis_pad)
            def _():
                at.stack[cut:cut + quarter, :] = at.self_rows[...]

        def stack_of(part):
            def block(place):
                return at.stack.at[pl.ds(pl.multiple_of(place * height + part * tall, tall), tall)]

            def region(count):
                return at.stack.at[pl.ds(0, count * tall)]

            return reduce_of(at.stack_reduce[part], DOM, dom, block, region)

        stacks = [stack_of(part) for part in range(rounds)]
        last_step = stacks[0].columns - 1
        def coef_start():
            at.scaled[...] = jnp.zeros((basis_rows, edges), F32)
            for chunk in range(chunks):
                lanes = pl.ds(chunk * span, span)
                grad = at.grad_message[:, lanes].astype(F32)
                for k in range(basis_count):
                    value = at.products[k * quarter:(k + 1) * quarter, lanes].astype(F32) * grad
                    at.scaled[k:k + 1, lanes] = jnp.sum(value, axis=0, keepdims=True)
            scaled = at.scaled[...]
            high = scaled.astype(BF)
            low = (scaled - high.astype(F32)).astype(BF)
            both = dot(jnp.concatenate([high, low], axis=0), at.rel_hot[...], 1, 1)
            coef_part = (both[:basis_rows] + both[basis_rows:]) * scale
            stacked = jnp.concatenate(
                [coef_part[:, k * LANES:(k + 1) * LANES] for k in range(rel_pad // LANES)], axis=0
            )
            at.coef_out[...] = stacked.reshape(dom, coef_rows, LANES)
            coef = Swap(
                DOM,
                dom,
                lambda place: at.coef_out.at[place],
                lambda place: at.coef_in.at[place],
                first_of(at.coef_in),
            at.coef_sems,
            )
            coef.start()
            at.coef_in[me] = at.coef_out[me]
            return coef

        if rotated:

            def work(step):
                stack = stacks[part]
                place = stack.place(step)
                other = (place * 2 + 1 - stack.side) * group + part * bunch
                mine = (place * 2 + stack.side) * group + part * bunch
                combine(other)
                stack.passing(step).start()
                combine(mine)

            part = 0
            work(0)
            coef = coef_start()
            each(1, last_step + 1, work)
            for part in range(1, rounds):
                each(0, last_step + 1, work)
        else:

            def whole(index, carry):
                combine(index * bunch)
                return carry

            coef = coef_start()
            lax.fori_loop(0, basis_pad // bunch, whole, 0)
            each(0, last_step + 1, lambda step: stacks[0].passing(step).start())

        edge = reduce_of(at.edge_reduce, FEAT, feat, lambda place: at.edge_send.at[place], first_of(at.edge_send))
        every = at.bases[...].reshape(total_rows, width)
        edge_sum = dot(every, at.combined[...], 0, 0).astype(BF)
        at.edge_send[...] = edge_sum.reshape(feat, quarter, edges)
        each(0, edge.columns, lambda step: edge.passing(step).start())
        each(0, self_reduce.columns - 1, self_reduce.middle)
        soon = min(2, last_step)
        each(0, soon, stacks[0].middle)
        each(0, edge.columns - 1, edge.middle)
        each(soon, last_step, stacks[0].middle)

        coef.wait_all()
        at.coef_feat[fme] = jnp.sum(at.coef_in[...], axis=0)
        coef_feat = Swap(
            FEAT,
            feat,
            lambda place: at.coef_feat.at[fme],
            lambda place: at.coef_feat.at[place],
            first_of(at.coef_feat),
            at.coef_feat_sems,
        )
        coef_feat.start()
        for stack in stacks[1:]:
            each(0, soon, stack.middle)

        self_reduce.finish(at.self_sum)
        edge.finish(at.edge_total)
        at.edge_grad[...] = at.edge_total[...].astype(BF)
        node = reduce_of(at.node_reduce, DOM, dom, lambda place: at.nodes.at[place], first_of(at.nodes))

        def scatter(place):
            at.nodes[place] = dot(at.edge_grad[...], hot_of(place), 1, 1).astype(BF)

        def spread(step):
            place = node.place(step)
            scatter(place * 2 + 1 - node.side)
            node.passing(step).start()
            scatter(place * 2 + node.side)

        def piece_of(part):
            rows_of = pl.ds(part * strip, strip)
            return Chain(
                DOM,
                dom,
                lambda place: pieces_ref.at[place, rows_of],
                lambda count: pieces_ref.at[pl.ds(0, count), rows_of],
                at.pieces_sems[part],
            )

        pieces = [piece_of(part) for part in range(parts)]

        def piece_pass(hop):
            for piece in pieces:
                piece.forward(hop)

        for stack in stacks[1:]:
            each(soon, last_step, stack.middle)
        coef_feat.wait_all()
        coef_all_ref[me] = jnp.sum(at.coef_feat[...], axis=0)
        coef_all = Swap(
            DOM,
            dom,
            lambda place: coef_all_ref.at[me],
            lambda place: coef_all_ref.at[place],
            first_of(coef_all_ref),
            at.coef_all_sems,
        )
        coef_all.start()
        each(0, node.columns, spread)
        stacks[0].finish(at.piece)
        pieces_ref[me] = (at.piece[...] * scale).astype(BF)
        for piece in pieces:
            piece.start()
        each(1, node.columns, piece_pass)
        each(0, node.columns - 1, node.middle)
        node.finish(at.node_sum)
        grad_feats_ref[...] = (at.self_sum[...] + at.node_sum[...]).astype(BF)
        for piece in pieces:
            each(0, piece.columns, lambda hop: piece.from_mate(hop))
        coef_all.wait_all()

        exchanges = [slot, own, message, back, coef, coef_feat, coef_all]
        for done in tables + exchanges + gathers + pieces:
            done.finish()
        for done in [self_reduce, edge, node] + stacks:
            done.drain()

    vmem = pl.BlockSpec(memory_space=pltpu.VMEM)
    output, grad_feats, pieces, coef_all = pl.pallas_call(
        kernel,
        out_shape=(
            jax.ShapeDtypeStruct((quarter, entities), BF),
            jax.ShapeDtypeStruct((quarter, entities), BF),
            jax.ShapeDtypeStruct((dom, height, width), BF),
            jax.ShapeDtypeStruct((dom, coef_rows, LANES), F32),
        ),
        in_specs=[pl.BlockSpec(memory_space=pltpu.HBM)] * 11,
        out_specs=(vmem,) * 4,
        scratch_shapes=shapes,
        compiler_params=pltpu.CompilerParams(
            collective_id=0, has_side_effects=True, vmem_limit_bytes=60 * 1024 * 1024
        ),
    )(bases, *given, owner, valid)

    step = group_of(basis_count)
    halves = rel_pad // LANES

    def last(output_in, feats_in, flat_in, coef_in, *outs):
        output_out, feats_out, bases_out, self_out, coef_out, wide, sem = outs
        copies = []
        for index in range(basis_count // step):
            spots = pl.ds(index * step, step)
            value = flat_in[index * step * quarter:(index + 1) * step * quarter, :]
            wide[spots] = value.astype(F32).reshape(step, quarter, width)
            copy = pltpu.make_async_copy(wide.at[spots], bases_out.at[spots], sem.at[index])
            copy.start()
            copies.append(copy)
        output_out[...] = output_in[...]
        feats_out[...] = feats_in[...]
        self_out[...] = flat_in[cut:cut + quarter, :].astype(F32)
        parts = [coef_in[k * basis_rows:(k + 1) * basis_rows] for k in range(halves)]
        coef_out[...] = jnp.concatenate(parts, axis=1)[:basis_count, :relations]
        for copy in copies:
            copy.wait()

    output, grad_feats, grad_bases, grad_self, grad_coef = pl.pallas_call(
        last,
        out_shape=(
            jax.ShapeDtypeStruct((quarter, entities), BF),
            jax.ShapeDtypeStruct((quarter, entities), BF),
            jax.ShapeDtypeStruct((basis_count, quarter, width), F32),
            jax.ShapeDtypeStruct((quarter, width), F32),
            jax.ShapeDtypeStruct((basis_count, relations), F32),
        ),
        in_specs=[vmem] * 4,
        out_specs=(vmem, vmem, pl.BlockSpec(memory_space=pl.ANY), vmem, vmem),
        scratch_shapes=[
            pltpu.VMEM((basis_count, quarter, width), F32),
            pltpu.SemaphoreType.DMA((basis_count // step,)),
        ],
    )(
        output,
        grad_feats,
        pieces.reshape(total_rows, width),
        coef_all.reshape(halves * basis_rows, LANES),
    )
    return output, grad_feats, grad_bases, grad_self.T, grad_coef.T


def body(
    feats,
    self_weight,
    bases,
    coef,
    src_part,
    src_row,
    edge_dst,
    edge_rel,
    block_owner,
    block_valid,
    cotangent,
):
    return layer(
        feats,
        self_weight.T,
        bases,
        coef.T,
        src_part.reshape(1, -1),
        src_row.reshape(1, -1),
        edge_dst.reshape(1, -1),
        edge_rel.reshape(1, -1),
        cotangent,
        block_owner.reshape(1, -1),
        block_valid,
        lax.axis_size(DOM),
        lax.axis_size(FEAT),
    )


def solution(mesh):
    return jax.shard_map(
        body,
        mesh=mesh,
        in_specs=(
            P(FEAT, DOM),
            P(None, FEAT),
            P(None, FEAT, None),
            P(),
            P(DOM, None),
            P(DOM),
            P(DOM),
            P(DOM),
            P(DOM, None),
            P(DOM, None),
            P(FEAT, DOM),
        ),
        out_specs=(P(FEAT, DOM), P(FEAT, DOM), P(None, FEAT, None), P(None, FEAT), P()),
        check_vma=False,
    )
```
